32 devices in a mesh: dp: 2 (over x), row: 4 (over z), col: 4 (over y, core).
Axes of the slice: x: 2, y: 2, z: 4, core: 2. Of those that a mesh axis runs over, the one named last changes fastest.
Arguments:
- x: bfloat16 [2048, 1024], P(('dp', 'row', 'col')), parts along dimension 0
- route_idx: int32 [2048, 8], P(('dp', 'row', 'col')), parts along dimension 0
- gates: float32 [2048, 8], P(('dp', 'row', 'col')), parts along dimension 0
- w1: bfloat16 [128, 1024, 384], P(('row', 'col'))
- w3: bfloat16 [128, 1024, 384], P(('row', 'col'))
- w2: bfloat16 [128, 384, 1024], P(('row', 'col'))
- dy: bfloat16 [2048, 1024], P(('dp', 'row', 'col')), parts along dimension 0
Outputs:
- output 1: bfloat16 [2048, 1024], P(('dp', 'row', 'col')), parts along dimension 0
- output 2: bfloat16 [2048, 1024], P(('dp', 'row', 'col')), parts along dimension 0
- output 3: float32 [2048, 8], P(('dp', 'row', 'col')), parts along dimension 0
- output 4: float32 [256, 1024, 384], P(('dp', 'row', 'col')), parts along dimension 0
- output 5: float32 [256, 1024, 384], P(('dp', 'row', 'col')), parts along dimension 0
- output 6: float32 [256, 384, 1024], P(('dp', 'row', 'col')), parts along dimension 0
There are 2 independent parts. The reference program is written for one: setup_inputs(seed, part) draws one part's arguments, and reference() takes and returns one part's arrays. A program takes and returns all parts, laid end to end along the dimension named above; an argument that names none is the same for every part.
All inputs are finite; a program needn't handle non-finite values.
Results may differ from the reference program's by a relative error of at most 0.00121.
Values are sent between devices in bfloat16 or wider.
A program may use at most 1 GiB of HBM per device.

```python
import jax
import jax.numpy as jnp
from jax import lax

TOK = 64
NDEV = 16
D = 1024
FF = 384
EXPERTS = 128
TOP = 8

TG = NDEV * TOK
CAP = (4 * TOK * TOP + EXPERTS - 1) // EXPERTS
CG = NDEV * CAP
NH = max(1, min(TOP // 2, (8 * TOP) // NDEV))
HOT = 2 * EXPERTS // NDEV
NCOLD = EXPERTS - HOT


def setup_inputs(seed: int = 0, part: int = 0) -> dict:
    kw = jax.random.split(jax.random.key(seed), 3)
    kp = jax.random.split(jax.random.fold_in(jax.random.key(seed + 1), part), 8)
    w1 = (jax.random.normal(kw[0], (EXPERTS, D, FF), jnp.float32) * D ** -0.5).astype(jnp.bfloat16)
    w3 = (jax.random.normal(kw[1], (EXPERTS, D, FF), jnp.float32) * D ** -0.5).astype(jnp.bfloat16)
    w2 = (jax.random.normal(kw[2], (EXPERTS, FF, D), jnp.float32) * FF ** -0.5).astype(jnp.bfloat16)
    dmax = min(NH, HOT - NH, TOP - NH)
    sh = jax.random.randint(kp[2], (), 0, HOT)
    sc = jax.random.randint(kp[3], (), 0, NCOLD)
    dd = jax.random.randint(kp[0], (NDEV, TOK // 2), 0, dmax + 1)
    nh = jnp.stack([NH + dd, NH - dd], axis=-1).reshape(NDEV, TOK)
    nc = TOP - nh
    sth = jnp.cumsum(nh, axis=1) - nh
    stc = jnp.cumsum(nc, axis=1) - nc
    dev = jnp.arange(NDEV)[:, None, None]
    j = jnp.arange(TOP)[None, None, :]
    hot_ids = (sh + dev * (TOK * NH) + sth[:, :, None] + j) % HOT
    cold_ids = HOT + (sc + dev * (TOK * (TOP - NH)) + stc[:, :, None] + j - nh[:, :, None]) % NCOLD
    ids = jnp.where(j < nh[:, :, None], hot_ids, cold_ids).reshape(TG, TOP)
    ids = jax.random.permutation(kp[4], ids, axis=1, independent=True).astype(jnp.int32)
    gu = jax.random.uniform(kp[5], (TG, TOP), jnp.float32, 0.5, 1.5)
    gates = gu / jnp.sum(gu, axis=1, keepdims=True)
    x = jax.random.normal(kp[6], (TG, D), jnp.float32).astype(jnp.bfloat16)
    dy = jax.random.normal(kp[7], (TG, D), jnp.float32).astype(jnp.bfloat16)
    return {'x': x, 'route_idx': ids, 'gates': gates, 'w1': w1, 'w3': w3, 'w2': w2, 'dy': dy}


def reference(x, route_idx, gates, w1, w3, w2, dy):
    n = TG * TOP
    ef = route_idx.reshape(n)
    order = jnp.argsort(ef, stable=True).astype(jnp.int32)
    es = ef[order]
    first = jnp.searchsorted(es, es, side='left').astype(jnp.int32)
    rank = jnp.arange(n, dtype=jnp.int32) - first
    tab = jnp.full((EXPERTS, CG), n, jnp.int32).at[es, rank].set(order)
    gf = gates.reshape(n)

    def body(carry, inp):
        y_acc, dx_acc, dg = carry
        te, a1, a3, a2 = inp
        valid = te < n
        ai = jnp.minimum(te, n - 1)
        tk = ai // TOP
        xr = x[tk]
        xs = jnp.where(valid[:, None], xr, jnp.zeros_like(xr))
        u = jnp.dot(xs, a1, preferred_element_type=jnp.float32).astype(jnp.bfloat16).astype(jnp.float32)
        v = jnp.dot(xs, a3, preferred_element_type=jnp.float32).astype(jnp.bfloat16).astype(jnp.float32)
        sg = jax.nn.sigmoid(u)
        a = (u * sg * v).astype(jnp.bfloat16)
        o = jnp.dot(a, a2, preferred_element_type=jnp.float32).astype(jnp.bfloat16).astype(jnp.float32)
        g = jnp.where(valid, gf[ai], 0.0)
        y_acc = y_acc.at[tk].add(g[:, None] * o)
        dys = dy[tk].astype(jnp.float32)
        dg = dg.at[ai].add(jnp.where(valid, jnp.sum(dys * o, axis=1), 0.0))
        do = (g[:, None] * dys).astype(jnp.bfloat16)
        gw2 = jnp.dot(a.T, do, preferred_element_type=jnp.float32)
        da = jnp.dot(do, a2.T, preferred_element_type=jnp.float32)
        du = (da * v * sg * (1.0 + u * (1.0 - sg))).astype(jnp.bfloat16)
        dv = (da * u * sg).astype(jnp.bfloat16)
        gw1 = jnp.dot(xs.T, du, preferred_element_type=jnp.float32)
        gw3 = jnp.dot(xs.T, dv, preferred_element_type=jnp.float32)
        dxs = jnp.dot(du, a1.T, preferred_element_type=jnp.float32) + jnp.dot(dv, a3.T, preferred_element_type=jnp.float32)
        dx_acc = dx_acc.at[tk].add(dxs.astype(jnp.bfloat16).astype(jnp.float32))
        return (y_acc, dx_acc, dg), (gw1, gw3, gw2)

    init = (jnp.zeros((TG, D), jnp.float32), jnp.zeros((TG, D), jnp.float32), jnp.zeros((n,), jnp.float32))
    (y_acc, dx_acc, dg), (gw1, gw3, gw2) = lax.scan(body, init, (tab, w1, w3, w2))
    return (y_acc.astype(jnp.bfloat16), dx_acc.astype(jnp.bfloat16), dg.reshape(TG, TOP), gw1, gw3, gw2)
```

```python
import functools

import jax
import jax.numpy as jnp
from jax import lax
from jax.experimental import pallas as pl
from jax.experimental.pallas import tpu as pltpu
from jax.sharding import PartitionSpec as P

TOK = 64
ND = 16
D = 1024
FF = 384
EL = 8
TOP = 8
CAP = 16
NB = 4
TB = 4 * TOK
RB = 4 * CAP
NT = ND * TOK
BF = jnp.bfloat16
F32 = jnp.float32
VMEM_LIMIT = 67043328


def dot(a, b):
    return lax.dot_general(a, b, (((1,), (0,)), ((), ())), preferred_element_type=F32)


def dot_nt(a, b):
    return lax.dot_general(a, b, (((1,), (1,)), ((), ())), preferred_element_type=F32)


def dot_tn(a, b):
    return lax.dot_general(a, b, (((0,), (0,)), ((), ())), preferred_element_type=F32)


def codes(base, route, gates, code, gate):
    rows = []
    for e in range(EL):
        eq = route == base + e
        rows.append(jnp.sum(jnp.where(eq, 1.0, 0.0), axis=0, keepdims=True))
        gate[e:e + 1, :] = jnp.sum(jnp.where(eq, gates, 0.0), axis=0, keepdims=True)
    mem = jnp.concatenate(rows, axis=0)
    i0 = lax.broadcasted_iota(jnp.int32, (TB, TB), 0)
    i1 = lax.broadcasted_iota(jnp.int32, (TB, TB), 1)
    upper = jnp.where((i0 < i1) & (i0 // TOK == i1 // TOK), 1.0, 0.0).astype(BF)
    src = lax.broadcasted_iota(jnp.int32, (EL, TB), 1) // TOK * CAP
    for b in range(NB):
        m = mem[:, b * TB:(b + 1) * TB]
        rank = dot(m.astype(BF), upper).astype(jnp.int32)
        code[:, b * TB:(b + 1) * TB] = jnp.where(m > 0.5, rank + src, -1)


def select(code, b):
    row = lax.broadcasted_iota(jnp.int32, (RB, TB), 0)
    c = code[:, pl.ds(b * TB, TB)]
    return jnp.concatenate([jnp.broadcast_to(c[e:e + 1], (RB, TB)) == row for e in range(EL)], axis=0)


def spread(gate, b):
    g = gate[:, pl.ds(b * TB, TB)]
    return jnp.concatenate([jnp.broadcast_to(g[e:e + 1], (RB, TB)) for e in range(EL)], axis=0)


def mid_kernel(route, gates, xg, dyg, w1h, w3h, w2h, yp, dxp, dgp, xr, dor, ar, dur, dvr,
               w1, w3, w2, code, gate, wsem, rows, orow, us, vs, gs, ds):
    for e in range(EL):
        pltpu.make_async_copy(w1h.at[e], w1.at[e], wsem.at[e, 0]).start()
        pltpu.make_async_copy(w3h.at[e], w3.at[e], wsem.at[e, 1]).start()
        pltpu.make_async_copy(w2h.at[e], w2.at[e], wsem.at[e, 2]).start()
    base = (lax.axis_index('row') * 4 + lax.axis_index('col')) * EL
    codes(base, route[...], gates[...], code, gate)

    def gather(src, dst):
        def body(b, _):
            p = jnp.where(select(code, b), 1.0, 0.0).astype(BF)
            dst[b] = dot(p, src[pl.ds(b * TB, TB), :]).astype(BF)
            return 0
        lax.fori_loop(0, NB, body, 0)

    def rows_of(ref, e):
        return ref[:, pl.ds(e * RB, RB), :]

    gather(xg, rows)

    def fwd(e, _):
        pltpu.make_async_copy(w1h.at[e], w1.at[e], wsem.at[e, 0]).wait()
        pltpu.make_async_copy(w3h.at[e], w3.at[e], wsem.at[e, 1]).wait()
        pltpu.make_async_copy(w2h.at[e], w2.at[e], wsem.at[e, 2]).wait()
        x = rows_of(rows, e).reshape(NB * RB, D)
        xr[e] = x
        u = dot(x, w1[e]).astype(BF)
        v = dot(x, w3[e]).astype(BF)
        us[e] = u
        vs[e] = v
        uf = u.astype(F32)
        a = (uf * jax.nn.sigmoid(uf) * v.astype(F32)).astype(BF)
        ar[e] = a
        orow[:, pl.ds(e * RB, RB), :] = dot(a, w2[e]).astype(BF).reshape(NB, RB, D)
        return 0

    lax.fori_loop(0, EL, fwd, 0)

    def scatter_y(b, _):
        w = jnp.where(select(code, b), spread(gate, b), 0.0)
        gs[b] = jnp.sum(w, axis=1, keepdims=True)
        hi = w.astype(BF)
        w = w - hi.astype(F32)
        mid = w.astype(BF)
        lo = (w - mid.astype(F32)).astype(BF)
        o = orow[b]
        yp[pl.ds(b * TB, TB), :] = dot_tn(hi, o) + dot_tn(mid, o) + dot_tn(lo, o)
        return 0

    lax.fori_loop(0, NB, scatter_y, 0)
    gather(dyg, rows)

    def bwd(e, _):
        dy = rows_of(rows, e).reshape(NB * RB, D).astype(F32)
        o = rows_of(orow, e).reshape(NB * RB, D).astype(F32)
        ds[:, pl.ds(e * RB, RB), :] = jnp.sum(dy * o, axis=1, keepdims=True).reshape(NB, RB, 1)
        g = gs[:, pl.ds(e * RB, RB), :].reshape(NB * RB, 1)
        do = (g * dy).astype(BF)
        dor[e] = do
        da = dot_nt(do, w2[e])
        u = us[e].astype(F32)
        v = vs[e].astype(F32)
        s = jax.nn.sigmoid(u)
        du = (da * v * s * (1.0 + u * (1.0 - s))).astype(BF)
        dv = (da * u * s).astype(BF)
        dur[e] = du
        dvr[e] = dv
        dx = (dot_nt(du, w1[e]) + dot_nt(dv, w3[e])).astype(BF)
        orow[:, pl.ds(e * RB, RB), :] = dx.reshape(NB, RB, D)
        return 0

    lax.fori_loop(0, EL, bwd, 0)

    def scatter_dx(b, _):
        sel = select(code, b)
        w = jnp.where(sel, 1.0, 0.0)
        dxp[pl.ds(b * TB, TB), :] = dot_tn(w.astype(BF), orow[b])
        dg = w * ds[b]
        for e in range(EL):
            dgp[pl.ds(e, 1), pl.ds(b * TB, TB)] = jnp.sum(dg[e * RB:(e + 1) * RB], axis=0, keepdims=True)
        return 0

    lax.fori_loop(0, NB, scatter_dx, 0)


def mid(route, gates, xg, dyg, w1, w3, w2):
    vm = pl.BlockSpec(memory_space=pltpu.VMEM)
    hb = pl.BlockSpec(memory_space=pl.ANY)
    sds = jax.ShapeDtypeStruct
    R = NB * RB
    return pl.pallas_call(
        mid_kernel,
        out_shape=(sds((NT, D), F32), sds((NT, D), F32), sds((EL, NT), F32),
                   sds((EL, R, D), BF), sds((EL, R, D), BF), sds((EL, R, FF), BF), sds((EL, R, FF), BF), sds((EL, R, FF), BF)),
        in_specs=[vm, vm, vm, vm, hb, hb, hb],
        out_specs=[vm] * 8,
        scratch_shapes=[
            pltpu.VMEM((EL, D, FF), BF), pltpu.VMEM((EL, D, FF), BF), pltpu.VMEM((EL, FF, D), BF),
            pltpu.VMEM((EL, NT), jnp.int32), pltpu.VMEM((EL, NT), F32),
            pltpu.SemaphoreType.DMA((EL, 3)),
            pltpu.VMEM((NB, EL * RB, D), BF), pltpu.VMEM((NB, EL * RB, D), BF),
            pltpu.VMEM((EL, R, FF), BF), pltpu.VMEM((EL, R, FF), BF),
            pltpu.VMEM((NB, EL * RB, 1), F32), pltpu.VMEM((NB, EL * RB, 1), F32),
        ],
        compiler_params=pltpu.CompilerParams(vmem_limit_bytes=VMEM_LIMIT),
        name='mid',
    )(route, gates, xg, dyg, w1, w3, w2)


def dw_kernel(x, do, a, du, dv, g1, g3, g2):
    xb = x[0]
    g1[0] = dot_tn(xb, du[0])
    g3[0] = dot_tn(xb, dv[0])
    g2[0] = dot_tn(a[0], do[0])


def dw(xr, dor, ar, dur, dvr):
    sds = jax.ShapeDtypeStruct
    R = NB * RB
    sp = lambda *s: pl.BlockSpec((1,) + s, lambda e: (e, 0, 0))
    return pl.pallas_call(
        dw_kernel,
        grid=(EL,),
        out_shape=(sds((EL, D, FF), F32), sds((EL, D, FF), F32), sds((EL, FF, D), F32)),
        in_specs=[sp(R, D), sp(R, D), sp(R, FF), sp(R, FF), sp(R, FF)],
        out_specs=[sp(D, FF), sp(D, FF), sp(FF, D)],
        name='dw',
    )(xr, dor, ar, dur, dvr)


def solution(mesh):
    grp = ('row', 'col')
    tspec = P(('dp', 'row', 'col'), None)
    wspec = P(grp, None, None)
    gspec = P(('dp', 'row', 'col'), None, None)

    def local(x, ridx, gates, w1, w3, w2, dy):
        meta = jnp.concatenate([ridx.astype(F32).T, gates.T])
        mg = lax.all_gather(meta, grp, axis=0).transpose(1, 0, 2).reshape(2 * TOP, NT)
        route = mg[:TOP].astype(jnp.int32)
        xg = lax.all_gather(x, grp, axis=0, tiled=True)
        dyg = lax.all_gather(dy, grp, axis=0, tiled=True)
        yp, dxp, dgp, xr, dor, ar, dur, dvr = mid(route, mg[TOP:], xg, dyg, w1, w3, w2)
        y = lax.psum_scatter(yp, grp, scatter_dimension=0, tiled=True).astype(BF)
        dx = lax.psum_scatter(dxp, grp, scatter_dimension=0, tiled=True).astype(BF)
        dgt = lax.all_to_all(dgp.reshape(EL, ND, TOK).transpose(1, 0, 2), grp, 0, 0, tiled=True).reshape(ND * EL, TOK)
        hit = ridx.T[None] == jnp.arange(ND * EL, dtype=jnp.int32)[:, None, None]
        dgates = jnp.sum(jnp.where(hit, dgt[:, None, :], 0.0), axis=0).T
        g1, g3, g2 = dw(xr, dor, ar, dur, dvr)
        return y, dx, dgates, g1, g3, g2

    return jax.shard_map(local, mesh=mesh, in_specs=(tspec, tspec, tspec, wspec, wspec, wspec, tspec),
                         out_specs=(tspec, tspec, tspec, gspec, gspec, gspec), check_vma=False)
```

```python
import functools

import jax
import jax.numpy as jnp
from jax import lax
from jax.experimental import pallas as pl
from jax.experimental.pallas import tpu as pltpu
from jax.sharding import PartitionSpec as P

TOK = 64
ND = 16
D = 1024
FF = 384
EL = 8
TOP = 8
CAP = 16
NB = 4
TB = 4 * TOK
RB = 4 * CAP
NT = ND * TOK
BF = jnp.bfloat16
F32 = jnp.float32
VMEM_LIMIT = 67043328


def dot(a, b):
    return lax.dot_general(a, b, (((1,), (0,)), ((), ())), preferred_element_type=F32)


def dot_nt(a, b):
    return lax.dot_general(a, b, (((1,), (1,)), ((), ())), preferred_element_type=F32)


def dot_tn(a, b):
    return lax.dot_general(a, b, (((0,), (0,)), ((), ())), preferred_element_type=F32)


def put_codes(b, base, meta, code, gate):
    m = [meta[NB * b + i] for i in range(NB)]
    route = jnp.concatenate([a[:TOP, :TOK] for a in m], axis=1)
    gates = jnp.concatenate([a[TOP:, :TOK] for a in m], axis=1)
    rows, gr = [], []
    for e in range(EL):
        eq = route == (base + e).astype(F32)
        rows.append(jnp.sum(jnp.where(eq, 1.0, 0.0), axis=0, keepdims=True))
        gr.append(jnp.sum(jnp.where(eq, gates, 0.0), axis=0, keepdims=True))
    mem = jnp.concatenate(rows, axis=0)
    gate[b] = jnp.concatenate(gr, axis=0)
    i0 = lax.broadcasted_iota(jnp.int32, (TB, TB), 0)
    i1 = lax.broadcasted_iota(jnp.int32, (TB, TB), 1)
    upper = jnp.where((i0 < i1) & (i0 // TOK == i1 // TOK), 1.0, 0.0).astype(BF)
    src = lax.broadcasted_iota(jnp.int32, (EL, TB), 1) // TOK * CAP
    rank = dot(mem.astype(BF), upper).astype(jnp.int32)
    code[b] = jnp.where(mem > 0.5, rank + src, -1)


def select(code, b):
    row = lax.broadcasted_iota(jnp.int32, (RB, TB), 0)
    c = code[b]
    return jnp.concatenate([jnp.broadcast_to(c[e:e + 1], (RB, TB)) == row for e in range(EL)], axis=0)


def spread(gate, b):
    g = gate[b]
    return jnp.concatenate([jnp.broadcast_to(g[e:e + 1], (RB, TB)) for e in range(EL)], axis=0)


def place(pos, core):
    y = pos // 4
    return pos + y * (7 - 2 * pos), 2 * y + core


def slot(pos, core):
    row, col = place(pos, core)
    return row * 4 + col


def remote(src, dst, ss, rs, dev):
    return pltpu.make_async_remote_copy(
        src_ref=src, dst_ref=dst, send_sem=ss, recv_sem=rs,
        device_id={'row': dev[0], 'col': dev[1]}, device_id_type=pl.DeviceIdType.MESH)


HALF = TOK // 2


def main_kernel(x, dy, meta, w1h, w3h, w2h, yo, dxo, dgo, xrh, dorh, arh, durh, dvrh,
                w1, w3, w2, wsem, osem, xg, dyg, mg, code, gate, xrow, dyrow, orow, us, vs, av, gs, ds,
                acc, pbuf, rbuf, dgs, dgr,
                ags, agr, pgs, pgr, ms, mr, gss, gsr, rss, rsr, rps, rpr):
    z = lax.axis_index('row')
    c4 = lax.axis_index('col')
    yy = c4 // 2
    core = c4 % 2
    r = z + yy * (7 - 2 * z)
    me = z * 4 + c4
    base = me * EL
    right, left = (r + 1) % 8, (r + 7) % 8
    nbr = (place(right, core), place(left, core))
    partner = (z, 2 * yy + 1 - core)

    def peer(o):
        q = (me + o) % ND
        return q, (q // 4, q % 4)

    barrier = pltpu.get_barrier_semaphore()

    def hello(o, _):
        q, dev = peer(o)
        pl.semaphore_signal(barrier, inc=1, device_id={'row': dev[0], 'col': dev[1]},
                            device_id_type=pl.DeviceIdType.MESH)
        return 0

    lax.fori_loop(1, ND, hello, 0)

    def load(e, _):
        pltpu.make_async_copy(w1h.at[e], w1.at[e], wsem.at[e, 0]).start()
        pltpu.make_async_copy(w3h.at[e], w3.at[e], wsem.at[e, 1]).start()
        pltpu.make_async_copy(w2h.at[e], w2.at[e], wsem.at[e, 2]).start()
        return 0

    lax.fori_loop(0, EL, load, 0)
    xg[me] = x[...]
    dyg[me] = dy[...]
    mg[me] = meta[...]
    pl.semaphore_wait(barrier, ND - 1)

    def meta_copy(o):
        q, dev = peer(o)
        return remote(meta, mg.at[me], ms.at[o], mr.at[o], dev)

    def meta_send(o, _):
        meta_copy(o).start()
        return 0

    def meta_wait(o, _):
        meta_copy(o).wait_recv()
        return 0

    lax.fori_loop(1, ND, meta_send, 0)

    gath = ((x, xg), (dy, dyg))

    def own(t, d, m, src=None):
        h = m if d == 0 else 1 - m
        return remote(gath[t][0].at[pl.ds(h * HALF, HALF)], gath[t][1].at[me, pl.ds(h * HALF, HALF)],
                      ags.at[t, d, m], agr.at[t, d, m], nbr[d])

    def chunk(t, d, m):
        k = 1 + m // 2
        h = m % 2 if d == 0 else 1 - m % 2
        p = slot((r + 8 - k) % 8 if d == 0 else (r + k) % 8, core)
        return gath[t][1].at[p, pl.ds(pl.multiple_of(h * HALF, HALF), HALF)]

    def onward(t, d, m):
        c = chunk(t, d, m)
        return remote(c, c, ags.at[t, d, m + 2], agr.at[t, d, m + 2], nbr[d])

    def across(t, d, m):
        c = chunk(t, d, m)
        return remote(c, c, pgs.at[t, d, m], pgr.at[t, d, m], partner)

    def own_across(t):
        return remote(gath[t][0], gath[t][1].at[me], pgs.at[t, 0, 7], pgr.at[t, 0, 7], partner)

    def ag_start(t):
        for m in range(2):
            for d in range(2):
                own(t, d, m).start()
        own_across(t).start()

    def ag_step(t, m):
        for d in range(2):
            c = chunk(t, d, m)
            remote(c, c, ags.at[t, d, m], agr.at[t, d, m], nbr[d]).wait_recv()

            @pl.when(m <= 4)
            def _():
                onward(t, d, m).start()
            across(t, d, m).start()

    def ag_wait_partner(t):
        def body(m, _):
            for d in range(2):
                across(t, d, m).wait_recv()
            return 0
        lax.fori_loop(0, 7, body, 0)
        own_across(t).wait_recv()

    def ag_drain(t):
        def body(m, _):
            for d in range(2):
                c = chunk(t, d, m)
                remote(c, c, ags.at[t, d, m], agr.at[t, d, m], nbr[d]).wait_send()
                across(t, d, m).wait_send()
            return 0
        lax.fori_loop(0, 7, body, 0)
        own_across(t).wait_send()

    ag_start(0)

    def xstep(m, _):
        ag_step(0, m)

        @pl.when(m == 1)
        def _():
            lax.fori_loop(1, ND, meta_wait, 0)

        @pl.when((m >= 2) & (m < 6))
        def _():
            put_codes(m - 2, base, mg, code, gate)
        return 0

    lax.fori_loop(0, 7, xstep, 0)
    ag_start(1)
    ag_wait_partner(0)

    def gather(src, dst):
        def body(b, _):
            p = jnp.where(select(code, b), 1.0, 0.0).astype(BF)
            dst[b] = dot(p, src[pl.ds(NB * b, NB)].reshape(TB, D)).astype(BF)
            return 0
        lax.fori_loop(0, NB, body, 0)

    def rows_of(ref, e):
        return ref[:, pl.ds(pl.multiple_of(e * RB, RB), RB), :]

    def put_rows(ref, e, v):
        ref[:, pl.ds(pl.multiple_of(e * RB, RB), RB), :] = v.reshape(NB, RB, v.shape[-1])

    gather(xg, xrow)
    out_x = pltpu.make_async_copy(xrow, xrh, osem.at[0])
    out_x.start()

    def fwd(e, _):
        pltpu.make_async_copy(w1h.at[e], w1.at[e], wsem.at[e, 0]).wait()
        pltpu.make_async_copy(w3h.at[e], w3.at[e], wsem.at[e, 1]).wait()
        pltpu.make_async_copy(w2h.at[e], w2.at[e], wsem.at[e, 2]).wait()
        xe = rows_of(xrow, e).reshape(NB * RB, D)
        u = dot(xe, w1[e]).astype(BF)
        v = dot(xe, w3[e]).astype(BF)
        us[e] = u
        vs[e] = v
        uf = u.astype(F32)
        a = (uf * jax.nn.sigmoid(uf) * v.astype(F32)).astype(BF)
        av[e] = a
        put_rows(orow, e, dot(a, w2[e]).astype(BF))

        @pl.when(e < 7)
        def _():
            ag_step(1, e)
        return 0

    lax.fori_loop(0, EL, fwd, 0)
    out_a = pltpu.make_async_copy(av, arh, osem.at[1])
    out_a.start()

    def rs_pair(t, o):
        d = (r + o) % 8
        return remote(acc.at[t, slot(d, 1 - core)], pbuf.at[t, o], rps.at[t, o], rpr.at[t, o], partner)

    def rs_pair_all(t):
        for o in (4, 3, 5, 2, 6, 1, 7, 0):
            rs_pair(t, o).start()

    def rs_join(t, o):
        rs_pair(t, o).wait_recv()
        p = slot((r + o) % 8, core)
        acc[t, p] = acc[t, p] + pbuf[t, o]

    def rs_move(t, d, m):
        dist = 4 - (m + 1) // 2
        h = m % 2 if d == 0 else 1 - m % 2
        p = slot((r + dist) % 8 if d == 0 else (r + 8 - dist) % 8, core)
        rows = pl.ds(pl.multiple_of(h * HALF, HALF), HALF)
        return p, rows, remote(acc.at[t, p, rows], rbuf.at[t, d, m], rss.at[t, d, m], rsr.at[t, d, m], nbr[d])

    def rs_first(t):
        rs_join(t, 4)
        for d in range(2):
            rs_move(t, d, 0)[2].start()
        rs_join(t, 3)
        rs_join(t, 5)
        for d in range(2):
            rs_move(t, d, 1)[2].start()
        for o in (2, 6, 1, 7, 0):
            rs_join(t, o)

    def rs_step(t, m):
        for d in range(2):
            rs_move(t, d, m - 2)[2].wait_recv()
            p, rows, copy = rs_move(t, d, m)
            acc[t, p, rows] = acc[t, p, rows] + rbuf[t, d, m - 2]
            copy.start()

    def rs_last(t, out):
        for m in (5, 6):
            for d in range(2):
                rs_move(t, d, m)[2].wait_recv()
        out[:HALF] = (acc[t, me, :HALF] + rbuf[t, 0, 6] + rbuf[t, 1, 5]).astype(BF)
        out[HALF:] = (acc[t, me, HALF:] + rbuf[t, 0, 5] + rbuf[t, 1, 6]).astype(BF)

    def rs_drain(t):
        def body(m, _):
            for d in range(2):
                rs_move(t, d, m)[2].wait_send()
            return 0
        lax.fori_loop(0, 7, body, 0)

        def pair(o, _):
            rs_pair(t, o).wait_send()
            return 0
        lax.fori_loop(0, 8, pair, 0)

    def scatter_y(b, _):
        w = jnp.where(select(code, b), spread(gate, b), 0.0)
        gs[b] = jnp.sum(w, axis=1, keepdims=True)
        hi = w.astype(BF)
        w = w - hi.astype(F32)
        mid = w.astype(BF)
        lo = (w - mid.astype(F32)).astype(BF)
        o = orow[b]
        acc[0, pl.ds(NB * b, NB)] = (dot_tn(hi, o) + dot_tn(mid, o) + dot_tn(lo, o)).reshape(NB, TOK, D)
        return 0

    lax.fori_loop(0, NB, scatter_y, 0)
    rs_pair_all(0)
    rs_first(0)
    ag_wait_partner(1)
    gather(dyg, dyrow)

    def bwd(e, _):
        dye = rows_of(dyrow, e).reshape(NB * RB, D).astype(F32)
        o = rows_of(orow, e).reshape(NB * RB, D).astype(F32)
        put_rows(ds, e, jnp.sum(dye * o, axis=1, keepdims=True))
        g = rows_of(gs, e).reshape(NB * RB, 1)
        do = (g * dye).astype(BF)
        put_rows(dyrow, e, do)
        da = dot_nt(do, w2[e])
        u = us[e].astype(F32)
        v = vs[e].astype(F32)
        s = jax.nn.sigmoid(u)
        du = (da * v * s * (1.0 + u * (1.0 - s))).astype(BF)
        dv = (da * u * s).astype(BF)
        us[e] = du
        vs[e] = dv
        put_rows(orow, e, (dot_nt(du, w1[e]) + dot_nt(dv, w3[e])).astype(BF))

        @pl.when(e % 2 == 1)
        def _():
            rs_step(0, 2 + e // 2)
        return 0

    lax.fori_loop(0, EL, bwd, 0)
    outs = [pltpu.make_async_copy(dyrow, dorh, osem.at[2]), pltpu.make_async_copy(us, durh, osem.at[3]),
            pltpu.make_async_copy(vs, dvrh, osem.at[4])]
    for c in outs:
        c.start()

    def scatter_dx(b, _):
        w = jnp.where(select(code, b), 1.0, 0.0)
        acc[1, pl.ds(NB * b, NB)] = dot_tn(w.astype(BF), orow[b]).reshape(NB, TOK, D)
        dg = w * ds[b]
        dge = jnp.concatenate([jnp.sum(dg[e * RB:(e + 1) * RB], axis=0, keepdims=True) for e in range(EL)], axis=0)
        for i in range(NB):
            dgs[NB * b + i, :, :TOK] = dge[:, i * TOK:(i + 1) * TOK]
        return 0

    lax.fori_loop(0, NB, scatter_dx, 0)
    rs_step(0, 6)
    rs_pair_all(1)

    def dg_copy(o):
        q, dev = peer(o)
        return remote(dgs.at[q], dgr.at[me], gss.at[o], gsr.at[o], dev)

    def dg_send(o, _):
        dg_copy(o).start()
        return 0

    lax.fori_loop(1, ND, dg_send, 0)
    dgr[me] = dgs[me]
    rs_first(1)
    rs_last(0, yo)

    def dg_wait(o, _):
        dg_copy(o).wait_recv()
        return 0

    lax.fori_loop(1, ND, dg_wait, 0)

    def xrs(m, _):
        rs_step(1, m)
        return 0

    lax.fori_loop(2, 7, xrs, 0)
    ident = lax.broadcasted_iota(jnp.int32, (ND * EL, 128), 0).astype(F32)
    back = dgr[...].reshape(ND * EL, 128)
    for j in range(TOP):
        dgo[j:j + 1] = jnp.sum(jnp.where(ident == meta[j:j + 1], back, 0.0), axis=0, keepdims=True)
    rs_last(1, dxo)

    def small_drain(o, _):
        meta_copy(o).wait_send()
        dg_copy(o).wait_send()
        return 0

    lax.fori_loop(1, ND, small_drain, 0)
    for t in range(2):
        ag_drain(t)
        rs_drain(t)
    out_x.wait()
    out_a.wait()
    for c in outs:
        c.wait()


def main(x, dy, meta, w1, w3, w2):
    vm = pl.BlockSpec(memory_space=pltpu.VMEM)
    hb = pl.BlockSpec(memory_space=pl.ANY)
    sds = jax.ShapeDtypeStruct
    R = NB * RB
    dma = lambda *s: pltpu.SemaphoreType.DMA(s)
    return pl.pallas_call(
        main_kernel,
        out_shape=(sds((TOK, D), BF), sds((TOK, D), BF), sds((TOP, 128), F32),
                   sds((NB, EL * RB, D), BF), sds((NB, EL * RB, D), BF), sds((EL, R, FF), BF), sds((EL, R, FF), BF), sds((EL, R, FF), BF)),
        in_specs=[vm, vm, vm, hb, hb, hb],
        out_specs=[vm, vm, vm] + [hb] * 5,
        scratch_shapes=[
            pltpu.VMEM((EL, D, FF), BF), pltpu.VMEM((EL, D, FF), BF), pltpu.VMEM((EL, FF, D), BF),
            dma(EL, 3), dma(5),
            pltpu.VMEM((ND, TOK, D), BF), pltpu.VMEM((ND, TOK, D), BF), pltpu.VMEM((ND, 2 * TOP, 128), F32),
            pltpu.VMEM((NB, EL, TB), jnp.int32), pltpu.VMEM((NB, EL, TB), F32),
            pltpu.VMEM((NB, EL * RB, D), BF), pltpu.VMEM((NB, EL * RB, D), BF), pltpu.VMEM((NB, EL * RB, D), BF),
            pltpu.VMEM((EL, R, FF), BF), pltpu.VMEM((EL, R, FF), BF), pltpu.VMEM((EL, R, FF), BF),
            pltpu.VMEM((NB, EL * RB, 1), F32), pltpu.VMEM((NB, EL * RB, 1), F32),
            pltpu.VMEM((2, ND, TOK, D), F32), pltpu.VMEM((2, 8, TOK, D), F32), pltpu.VMEM((2, 2, 7, HALF, D), F32),
            pltpu.VMEM((ND, EL, 128), F32), pltpu.VMEM((ND, EL, 128), F32),
            dma(2, 2, 7), dma(2, 2, 7), dma(2, 2, 8), dma(2, 2, 8), dma(ND), dma(ND), dma(ND), dma(ND),
            dma(2, 2, 7), dma(2, 2, 7), dma(2, 8), dma(2, 8),
        ],
        compiler_params=pltpu.CompilerParams(vmem_limit_bytes=VMEM_LIMIT, collective_id=0, has_side_effects=True),
        name='moe',
    )(x, dy, meta, w1, w3, w2)


def dw_kernel(x, do, a, du, dv, g1, g3, g2):
    xb = x[...].reshape(NB * RB, D)
    g1[0] = dot_tn(xb, du[0])
    g3[0] = dot_tn(xb, dv[0])
    g2[0] = dot_tn(a[0], do[...].reshape(NB * RB, D))


def dw(xr, dor, ar, dur, dvr):
    sds = jax.ShapeDtypeStruct
    R = NB * RB
    sp = lambda *s: pl.BlockSpec((1,) + s, lambda e: (e, 0, 0))
    br = pl.BlockSpec((NB, RB, D), lambda e: (0, e, 0))
    return pl.pallas_call(
        dw_kernel,
        grid=(EL,),
        out_shape=(sds((EL, D, FF), F32), sds((EL, D, FF), F32), sds((EL, FF, D), F32)),
        in_specs=[br, br, sp(R, FF), sp(R, FF), sp(R, FF)],
        out_specs=[sp(D, FF), sp(D, FF), sp(FF, D)],
        name='dw',
    )(xr, dor, ar, dur, dvr)


def solution(mesh):
    grp = ('row', 'col')
    tspec = P(('dp', 'row', 'col'), None)
    wspec = P(grp, None, None)
    gspec = P(('dp', 'row', 'col'), None, None)

    def local(x, ridx, gates, w1, w3, w2, dy):
        meta = jnp.pad(jnp.concatenate([ridx.astype(F32), gates], axis=1).T, ((0, 0), (0, 128 - TOK)))
        y, dx, dgt, xr, dor, ar, dur, dvr = main(x, dy, meta, w1, w3, w2)
        g1, g3, g2 = dw(xr, dor, ar, dur, dvr)
        return y, dx, dgt[:, :TOK].T, g1, g3, g2

    return jax.shard_map(local, mesh=mesh, in_specs=(tspec, tspec, tspec, wspec, wspec, wspec, tspec),
                         out_specs=(tspec, tspec, tspec, gspec, gspec, gspec), check_vma=False)
```

```python
import functools

import jax
import jax.numpy as jnp
from jax import lax
from jax.experimental import pallas as pl
from jax.experimental.pallas import tpu as pltpu
from jax.sharding import PartitionSpec as P

TOK = 64
ND = 16
D = 1024
FF = 384
EL = 8
TOP = 8
CAP = 16
NB = 4
TB = 4 * TOK
RB = 4 * CAP
NT = ND * TOK
BF = jnp.bfloat16
F32 = jnp.float32
VMEM_LIMIT = 67043328


def dot(a, b):
    return lax.dot_general(a, b, (((1,), (0,)), ((), ())), preferred_element_type=F32)


def dot_nt(a, b):
    return lax.dot_general(a, b, (((1,), (1,)), ((), ())), preferred_element_type=F32)


def dot_tn(a, b):
    return lax.dot_general(a, b, (((0,), (0,)), ((), ())), preferred_element_type=F32)


def put_codes(b, base, meta, code, gate):
    m = [meta[NB * b + i] for i in range(NB)]
    route = jnp.concatenate([a[:TOP, :TOK] for a in m], axis=1)
    gates = jnp.concatenate([a[TOP:, :TOK] for a in m], axis=1)
    rows, gr = [], []
    for e in range(EL):
        eq = route == (base + e).astype(F32)
        rows.append(jnp.sum(jnp.where(eq, 1.0, 0.0), axis=0, keepdims=True))
        gr.append(jnp.sum(jnp.where(eq, gates, 0.0), axis=0, keepdims=True))
    mem = jnp.concatenate(rows, axis=0)
    gate[b] = jnp.concatenate(gr, axis=0)
    i0 = lax.broadcasted_iota(jnp.int32, (TB, TB), 0)
    i1 = lax.broadcasted_iota(jnp.int32, (TB, TB), 1)
    upper = jnp.where((i0 < i1) & (i0 // TOK == i1 // TOK), 1.0, 0.0).astype(BF)
    src = lax.broadcasted_iota(jnp.int32, (EL, TB), 1) // TOK * CAP
    rank = dot(mem.astype(BF), upper).astype(jnp.int32)
    code[b] = jnp.where(mem > 0.5, rank + src, -1)


def select(code, b):
    row = lax.broadcasted_iota(jnp.int32, (RB, TB), 0)
    c = code[b]
    return jnp.concatenate([jnp.broadcast_to(c[e:e + 1], (RB, TB)) == row for e in range(EL)], axis=0)


def spread(gate, b):
    g = gate[b]
    return jnp.concatenate([jnp.broadcast_to(g[e:e + 1], (RB, TB)) for e in range(EL)], axis=0)


def put_tables(b, code, gate, gs, tab):
    lane = lax.broadcasted_iota(jnp.int32, (EL, EL * RB), 1)
    widen = jnp.where(lane // RB == lax.broadcasted_iota(jnp.int32, (EL, EL * RB), 0), 1.0, 0.0).astype(BF)
    row = (lax.broadcasted_iota(jnp.int32, (TB, EL * RB), 1) % RB).astype(F32)
    sel = dot_tn(code[b].astype(F32).astype(BF), widen) == row
    g = gate[b]
    for i in range(3):
        part = g.astype(BF)
        g = g - part.astype(F32)
        tab[b, i] = jnp.where(sel, dot_tn(part, widen), 0.0).astype(BF)
    tab[b, 3] = jnp.where(sel, 1.0, 0.0).astype(BF)
    gs[b] = jnp.sum(jnp.where(select(code, b), spread(gate, b), 0.0), axis=1, keepdims=True)


def place(pos, core):
    y = pos // 4
    return pos + y * (7 - 2 * pos), 2 * y + core


def slot(pos, core):
    row, col = place(pos, core)
    return row * 4 + col


def remote(src, dst, ss, rs, dev):
    return pltpu.make_async_remote_copy(
        src_ref=src, dst_ref=dst, send_sem=ss, recv_sem=rs,
        device_id={'row': dev[0], 'col': dev[1]}, device_id_type=pl.DeviceIdType.MESH)


HALF = TOK // 2
NC = 4
CH = TOK // NC
LAST = 3 * NC + NC // 2
DH = D // 2


def main_kernel(ridx, gates, x, dy, w1h, w3h, w2h, yo, dxo, dgo, xrh, dorh, arh, durh, dvrh,
                w1, w3, w2, wsem, osem, isem, meta, xg, dyg, mg, code, gate, tab, xrow, orow, us, vs, av, gs, ds,
                acc, pbuf, rbuf, dgs, dgr,
                ags, agr, pgs, pgr, ms, mr, gss, gsr, rss, rsr, rps, rpr):
    z = lax.axis_index('row')
    c4 = lax.axis_index('col')
    yy = c4 // 2
    core = c4 % 2
    r = z + yy * (7 - 2 * z)
    me = z * 4 + c4
    base = me * EL
    right, left = (r + 1) % 8, (r + 7) % 8
    nbr = (place(right, core), place(left, core))
    partner = (z, 2 * yy + 1 - core)

    def peer(o):
        q = (me + o) % ND
        return q, (q // 4, q % 4)

    in_x = pltpu.make_async_copy(x, xg.at[me], isem.at[0])
    in_dy = pltpu.make_async_copy(dy, dyg.at[me], isem.at[1])
    in_x.start()
    in_dy.start()
    barrier = pltpu.get_barrier_semaphore()

    def hello(o, _):
        q, dev = peer(o)
        pl.semaphore_signal(barrier, inc=1, device_id={'row': dev[0], 'col': dev[1]},
                            device_id_type=pl.DeviceIdType.MESH)
        return 0

    lax.fori_loop(1, ND, hello, 0)

    def load(e, _):
        pltpu.make_async_copy(w1h.at[e], w1.at[e], wsem.at[e, 0]).start()
        pltpu.make_async_copy(w3h.at[e], w3.at[e], wsem.at[e, 1]).start()
        pltpu.make_async_copy(w2h.at[e], w2.at[e], wsem.at[e, 2]).start()
        return 0

    lax.fori_loop(0, EL, load, 0)
    both = jnp.concatenate([ridx[...].astype(F32), gates[...], jnp.zeros((TOK, 128 - 2 * TOP), F32)], axis=1)
    turned = jnp.concatenate([both, jnp.zeros((128 - TOK, 128), F32)], axis=0).T
    meta[...] = turned[:2 * TOP]
    mg[me] = turned[:2 * TOP]
    in_x.wait()
    in_dy.wait()
    pl.semaphore_wait(barrier, ND - 1)

    def meta_copy(o):
        q, dev = peer(o)
        return remote(meta, mg.at[me], ms.at[o], mr.at[o], dev)

    def meta_send(o, _):
        meta_copy(o).start()
        return 0

    def meta_wait(o, _):
        meta_copy(o).wait_recv()
        return 0

    lax.fori_loop(1, ND, meta_send, 0)

    gath = (xg, dyg)

    def own(t, d, m):
        h = m if d == 0 else NC - 1 - m
        c = gath[t].at[me, pl.ds(h * CH, CH)]
        return remote(c, c, ags.at[t, d, m], agr.at[t, d, m], nbr[d])

    def chunk(t, d, m):
        k = 1 + m // NC
        h = m % NC if d == 0 else NC - 1 - m % NC
        p = slot((r + 8 - k) % 8 if d == 0 else (r + k) % 8, core)
        return gath[t].at[p, pl.ds(pl.multiple_of(h * CH, CH), CH)]

    def onward(t, d, m):
        c = chunk(t, d, m)
        return remote(c, c, ags.at[t, d, m + NC], agr.at[t, d, m + NC], nbr[d])

    def across(t, d, m):
        c = chunk(t, d, m)
        return remote(c, c, pgs.at[t, d, m], pgr.at[t, d, m], partner)

    def own_across(t):
        c = gath[t].at[me]
        return remote(c, c, pgs.at[t, 0, LAST], pgr.at[t, 0, LAST], partner)

    def ag_start(t):
        for m in range(NC):
            for d in range(2):
                own(t, d, m).start()
        own_across(t).start()

    def ag_step(t, m):
        for d in range(2):
            c = chunk(t, d, m)
            remote(c, c, ags.at[t, d, m], agr.at[t, d, m], nbr[d]).wait_recv()

            @pl.when(m < LAST - NC)
            def _():
                onward(t, d, m).start()
            across(t, d, m).start()

    def ag_wait_partner(t):
        def body(m, _):
            for d in range(2):
                across(t, d, m).wait_recv()
            return 0
        lax.fori_loop(0, LAST, body, 0)
        own_across(t).wait_recv()

    def ag_drain(t):
        def body(m, _):
            for d in range(2):
                c = chunk(t, d, m)
                remote(c, c, ags.at[t, d, m], agr.at[t, d, m], nbr[d]).wait_send()
                across(t, d, m).wait_send()
            return 0
        lax.fori_loop(0, LAST, body, 0)
        own_across(t).wait_send()

    ag_start(0)

    def xstep(m, _):
        ag_step(0, m)

        @pl.when(m == 1)
        def _():
            lax.fori_loop(1, ND, meta_wait, 0)

        @pl.when((m >= 2) & (m < 10) & (m % 2 == 0))
        def _():
            put_codes(m // 2 - 1, base, mg, code, gate)

        @pl.when((m >= 3) & (m < 11) & (m % 2 == 1))
        def _():
            put_tables(m // 2 - 1, code, gate, gs, tab)
        return 0

    lax.fori_loop(0, LAST, xstep, 0)
    ag_start(1)
    ag_wait_partner(0)

    def gather(src, dst):
        def body(b, _):
            p = jnp.where(select(code, b), 1.0, 0.0).astype(BF)
            dst[b] = dot(p, src[pl.ds(NB * b, NB)].reshape(TB, D)).astype(BF)
            return 0
        lax.fori_loop(0, NB, body, 0)

    def rows_of(ref, e):
        return ref[:, pl.ds(pl.multiple_of(e * RB, RB), RB), :]

    def put_rows(ref, e, v):
        ref[:, pl.ds(pl.multiple_of(e * RB, RB), RB), :] = v.reshape(NB, RB, v.shape[-1])

    gather(xg, xrow)
    out_x = pltpu.make_async_copy(xrow, xrh, osem.at[0])
    out_x.start()

    def fwd(e, _):
        pltpu.make_async_copy(w1h.at[e], w1.at[e], wsem.at[e, 0]).wait()
        pltpu.make_async_copy(w3h.at[e], w3.at[e], wsem.at[e, 1]).wait()
        xe = rows_of(xrow, e).reshape(NB * RB, D)
        u = dot(xe, w1[e]).astype(BF)
        v = dot(xe, w3[e]).astype(BF)
        us[e] = u
        vs[e] = v
        uf = u.astype(F32)
        av[e] = (uf * jax.nn.sigmoid(uf) * v.astype(F32)).astype(BF)
        ag_step(1, e)
        return 0

    lax.fori_loop(0, EL, fwd, 0)
    out_a = pltpu.make_async_copy(av, arh, osem.at[1])
    out_a.start()

    def rs_pair(t, o):
        d = (r + o) % 8
        return remote(acc.at[t, slot(d, 1 - core)], pbuf.at[t, o], rps.at[t, o], rpr.at[t, o], partner)

    def rs_pair_block(t, b):
        for d in (b, 7 - b):
            rs_pair(t, (d + 8 - r) % 8).start()

    def rs_join(t, o):
        rs_pair(t, o).wait_recv()
        p = slot((r + o) % 8, core)
        acc[t, p] = acc[t, p] + pbuf[t, o]

    def rs_move(t, d, m):
        dist = 4 - (m + 1) // 2
        h = m % 2 if d == 0 else 1 - m % 2
        p = slot((r + dist) % 8 if d == 0 else (r + 8 - dist) % 8, core)
        rows = pl.ds(pl.multiple_of(h * HALF, HALF), HALF)
        return p, rows, remote(acc.at[t, p, rows], rbuf.at[t, d, m], rss.at[t, d, m], rsr.at[t, d, m], nbr[d])

    def rs_first(t):
        rs_join(t, 4)
        for d in range(2):
            rs_move(t, d, 0)[2].start()
        rs_join(t, 3)
        rs_join(t, 5)
        for d in range(2):
            rs_move(t, d, 1)[2].start()
        for o in (2, 6, 1, 7, 0):
            rs_join(t, o)

    def rs_step(t, m):
        for d in range(2):
            rs_move(t, d, m - 2)[2].wait_recv()
            p, rows, copy = rs_move(t, d, m)
            acc[t, p, rows] = acc[t, p, rows] + rbuf[t, d, m - 2]
            copy.start()

    def rs_last(t, out):
        cols = slice((t % 2) * DH, (t % 2) * DH + DH)
        for m in (5, 6):
            for d in range(2):
                rs_move(t, d, m)[2].wait_recv()
        out[:HALF, cols] = (acc[t, me, :HALF] + rbuf[t, 0, 6] + rbuf[t, 1, 5]).astype(BF)
        out[HALF:, cols] = (acc[t, me, HALF:] + rbuf[t, 0, 5] + rbuf[t, 1, 6]).astype(BF)

    def rs_drain(t):
        def body(m, _):
            for d in range(2):
                rs_move(t, d, m)[2].wait_send()
            return 0
        lax.fori_loop(0, 7, body, 0)

        def pair(o, _):
            rs_pair(t, o).wait_send()
            return 0
        lax.fori_loop(0, 8, pair, 0)

    def forward_half(c):
        cols = slice(c * DH, c * DH + DH)

        def out(e, _):
            if c == 0:
                pltpu.make_async_copy(w2h.at[e], w2.at[e], wsem.at[e, 2]).wait()
            orow[:, pl.ds(pl.multiple_of(e * RB, RB), RB), cols] = dot(av[e], w2[e, :, cols]).astype(BF).reshape(NB, RB, DH)
            return 0

        lax.fori_loop(0, EL, out, 0)

        def scatter(i, _):
            b = (3 - z + i) % NB
            o = orow[b, :, cols]
            acc[c, pl.ds(NB * b, NB)] = (dot(tab[b, 0], o) + dot(tab[b, 1], o) + dot(tab[b, 2], o)).reshape(NB, TOK, DH)
            rs_pair_block(c, b)
            if c == 0:
                @pl.when(i < 3)
                def _():
                    ag_step(1, EL + 2 * i)
                    ag_step(1, EL + 2 * i + 1)
            return 0

        lax.fori_loop(0, NB, scatter, 0)
        rs_first(c)

    forward_half(0)
    forward_half(1)
    rs_step(0, 2)
    ag_wait_partner(1)
    out_x.wait()
    gather(dyg, xrow)

    def bwd(e, _):
        dye = rows_of(xrow, e).reshape(NB * RB, D).astype(F32)
        o = rows_of(orow, e).reshape(NB * RB, D).astype(F32)
        put_rows(ds, e, jnp.sum(dye * o, axis=1, keepdims=True))
        g = rows_of(gs, e).reshape(NB * RB, 1)
        do = (g * dye).astype(BF)
        put_rows(xrow, e, do)
        da = dot_nt(do, w2[e])
        u = us[e].astype(F32)
        v = vs[e].astype(F32)
        s = jax.nn.sigmoid(u)
        du = (da * v * s * (1.0 + u * (1.0 - s))).astype(BF)
        dv = (da * u * s).astype(BF)
        us[e] = du
        vs[e] = dv
        put_rows(orow, e, (dot_nt(du, w1[e]) + dot_nt(dv, w3[e])).astype(BF))

        @pl.when(e < 7)
        def _():
            i = e + 1
            rs_step((i // 2) % 2, 2 + 2 * (i // 4) + i % 2)
        return 0

    lax.fori_loop(0, EL, bwd, 0)
    outs = [pltpu.make_async_copy(xrow, dorh, osem.at[2]), pltpu.make_async_copy(us, durh, osem.at[3]),
            pltpu.make_async_copy(vs, dvrh, osem.at[4])]
    for c in outs:
        c.start()
    rs_step(0, 6)

    def backward_half(c):
        cols = slice(c * DH, c * DH + DH)

        def scatter(i, _):
            b = (3 - z + i) % NB
            acc[2 + c, pl.ds(NB * b, NB)] = dot(tab[b, 3], orow[b, :, cols]).reshape(NB, TOK, DH)
            rs_pair_block(2 + c, b)
            return 0

        lax.fori_loop(0, NB, scatter, 0)
        rs_first(2 + c)

    backward_half(0)
    rs_step(1, 6)
    backward_half(1)

    def slots_back(b, _):
        dg = jnp.where(select(code, b), ds[b], 0.0)
        dge = jnp.concatenate([jnp.sum(dg[e * RB:(e + 1) * RB], axis=0, keepdims=True) for e in range(EL)], axis=0)
        for i in range(NB):
            dgs[NB * b + i, :, :TOK] = dge[:, i * TOK:(i + 1) * TOK]
        return 0

    lax.fori_loop(0, NB, slots_back, 0)

    def dg_copy(o):
        q, dev = peer(o)
        return remote(dgs.at[q], dgr.at[me], gss.at[o], gsr.at[o], dev)

    def dg_send(o, _):
        dg_copy(o).start()
        return 0

    lax.fori_loop(1, ND, dg_send, 0)
    dgr[me] = dgs[me]
    rs_step(2, 2)
    rs_step(2, 3)
    rs_step(3, 2)
    rs_last(0, yo)
    rs_step(3, 3)
    rs_last(1, yo)
    rs_step(2, 4)

    def dg_wait(o, _):
        dg_copy(o).wait_recv()
        return 0

    lax.fori_loop(1, ND, dg_wait, 0)
    rs_step(2, 5)
    expert = lax.broadcasted_iota(jnp.int32, (TOK, ND * EL), 1)
    back = dgr[...].reshape(ND * EL, 128).T[:TOK]
    dgo[...] = jnp.concatenate(
        [jnp.sum(jnp.where(expert == ridx[:, j:j + 1], back, 0.0), axis=1, keepdims=True) for j in range(TOP)], axis=1)
    rs_step(3, 4)
    rs_step(3, 5)
    rs_step(2, 6)
    rs_step(3, 6)
    rs_last(2, dxo)
    rs_last(3, dxo)

    def small_drain(o, _):
        meta_copy(o).wait_send()
        dg_copy(o).wait_send()
        return 0

    lax.fori_loop(1, ND, small_drain, 0)
    for t in range(2):
        ag_drain(t)
    for t in range(4):
        rs_drain(t)
    out_a.wait()
    for c in outs:
        c.wait()


def main(ridx, gates, x, dy, w1, w3, w2):
    vm = pl.BlockSpec(memory_space=pltpu.VMEM)
    hb = pl.BlockSpec(memory_space=pl.ANY)
    sds = jax.ShapeDtypeStruct
    R = NB * RB
    dma = lambda *s: pltpu.SemaphoreType.DMA(s)
    return pl.pallas_call(
        main_kernel,
        out_shape=(sds((TOK, D), BF), sds((TOK, D), BF), sds((TOK, TOP), F32),
                   sds((NB, EL * RB, D), BF), sds((NB, EL * RB, D), BF), sds((EL, R, FF), BF), sds((EL, R, FF), BF), sds((EL, R, FF), BF)),
        in_specs=[vm, vm, hb, hb, hb, hb, hb],
        out_specs=[vm, vm, vm] + [hb] * 5,
        scratch_shapes=[
            pltpu.VMEM((EL, D, FF), BF), pltpu.VMEM((EL, D, FF), BF), pltpu.VMEM((EL, FF, D), BF),
            dma(EL, 3), dma(5), dma(2), pltpu.VMEM((2 * TOP, 128), F32),
            pltpu.VMEM((ND, TOK, D), BF), pltpu.VMEM((ND, TOK, D), BF), pltpu.VMEM((ND, 2 * TOP, 128), F32),
            pltpu.VMEM((NB, EL, TB), jnp.int32), pltpu.VMEM((NB, EL, TB), F32), pltpu.VMEM((NB, 4, TB, EL * RB), BF),
            pltpu.VMEM((NB, EL * RB, D), BF), pltpu.VMEM((NB, EL * RB, D), BF),
            pltpu.VMEM((EL, R, FF), BF), pltpu.VMEM((EL, R, FF), BF), pltpu.VMEM((EL, R, FF), BF),
            pltpu.VMEM((NB, EL * RB, 1), F32), pltpu.VMEM((NB, EL * RB, 1), F32),
            pltpu.VMEM((4, ND, TOK, DH), F32), pltpu.VMEM((4, 8, TOK, DH), F32), pltpu.VMEM((4, 2, 7, HALF, DH), F32),
            pltpu.VMEM((ND, EL, 128), F32), pltpu.VMEM((ND, EL, 128), F32),
            dma(2, 2, LAST), dma(2, 2, LAST), dma(2, 2, LAST + 1), dma(2, 2, LAST + 1), dma(ND), dma(ND), dma(ND), dma(ND),
            dma(4, 2, 7), dma(4, 2, 7), dma(4, 8), dma(4, 8),
        ],
        compiler_params=pltpu.CompilerParams(vmem_limit_bytes=VMEM_LIMIT, collective_id=0, has_side_effects=True),
        name='moe',
    )(ridx, gates, x, dy, w1, w3, w2)


def dw_kernel(y, dx, dg, x, do, a, du, dv, yo, dxo, dgo, g1, g3, g2):
    @pl.when((pl.program_id(0) == 0) & (pl.program_id(1) == 0))
    def _():
        yo[...] = y[...]
        dxo[...] = dx[...]
        dgo[...] = dg[...]
    xb = x[...].reshape(NB * RB, DH)
    g1[0] = dot_tn(xb, du[0])
    g3[0] = dot_tn(xb, dv[0])
    g2[0] = dot_tn(a[0], do[...].reshape(NB * RB, DH))


def dw(y, dx, dg, xr, dor, ar, dur, dvr):
    sds = jax.ShapeDtypeStruct
    R = NB * RB
    whole = lambda *s: pl.BlockSpec(s, lambda e, h: (0, 0))
    act = pl.BlockSpec((1, R, FF), lambda e, h: (e, 0, 0))
    br = pl.BlockSpec((NB, RB, DH), lambda e, h: (0, e, h))
    same = [whole(TOK, D), whole(TOK, D), whole(TOK, TOP)]
    return pl.pallas_call(
        dw_kernel,
        grid=(EL, 2),
        out_shape=(sds((TOK, D), BF), sds((TOK, D), BF), sds((TOK, TOP), F32),
                   sds((EL, D, FF), F32), sds((EL, D, FF), F32), sds((EL, FF, D), F32)),
        in_specs=same + [br, br, act, act, act],
        out_specs=same + [pl.BlockSpec((1, DH, FF), lambda e, h: (e, h, 0)), pl.BlockSpec((1, DH, FF), lambda e, h: (e, h, 0)),
                          pl.BlockSpec((1, FF, DH), lambda e, h: (e, 0, h))],
        name='dw',
    )(y, dx, dg, xr, dor, ar, dur, dvr)


def solution(mesh):
    grp = ('row', 'col')
    tspec = P(('dp', 'row', 'col'), None)
    wspec = P(grp, None, None)
    gspec = P(('dp', 'row', 'col'), None, None)

    def local(x, ridx, gates, w1, w3, w2, dy):
        return dw(*main(ridx, gates, x, dy, w1, w3, w2))

    return jax.shard_map(local, mesh=mesh, in_specs=(tspec, tspec, tspec, wspec, wspec, wspec, tspec),
                         out_specs=(tspec, tspec, tspec, gspec, gspec, gspec), check_vma=False)
```

```python
import functools

import jax
import jax.numpy as jnp
from jax import lax
from jax.experimental import pallas as pl
from jax.experimental.pallas import tpu as pltpu
from jax.sharding import PartitionSpec as P

TOK = 64
ND = 16
D = 1024
FF = 384
EL = 8
TOP = 8
CAP = 16
NB = 4
TB = 4 * TOK
RB = 4 * CAP
NT = ND * TOK
BF = jnp.bfloat16
F32 = jnp.float32
VMEM_LIMIT = 67043328


def dot(a, b):
    return lax.dot_general(a, b, (((1,), (0,)), ((), ())), preferred_element_type=F32)


def dot_nt(a, b):
    return lax.dot_general(a, b, (((1,), (1,)), ((), ())), preferred_element_type=F32)


def dot_tn(a, b):
    return lax.dot_general(a, b, (((0,), (0,)), ((), ())), preferred_element_type=F32)


def put_codes(b, base, meta, code, gate):
    m = [meta[NB * b + i] for i in range(NB)]
    route = jnp.concatenate([a[:TOP, :TOK] for a in m], axis=1)
    gates = jnp.concatenate([a[TOP:, :TOK] for a in m], axis=1)
    rows, gr = [], []
    for e in range(EL):
        eq = route == (base + e).astype(F32)
        rows.append(jnp.sum(jnp.where(eq, 1.0, 0.0), axis=0, keepdims=True))
        gr.append(jnp.sum(jnp.where(eq, gates, 0.0), axis=0, keepdims=True))
    mem = jnp.concatenate(rows, axis=0)
    gate[b] = jnp.concatenate(gr, axis=0)
    i0 = lax.broadcasted_iota(jnp.int32, (TB, TB), 0)
    i1 = lax.broadcasted_iota(jnp.int32, (TB, TB), 1)
    upper = jnp.where((i0 < i1) & (i0 // TOK == i1 // TOK), 1.0, 0.0).astype(BF)
    src = lax.broadcasted_iota(jnp.int32, (EL, TB), 1) // TOK * CAP
    rank = dot(mem.astype(BF), upper).astype(jnp.int32)
    code[b] = jnp.where(mem > 0.5, rank + src, -1)


def select(code, b):
    row = lax.broadcasted_iota(jnp.int32, (RB, TB), 0)
    c = code[b]
    return jnp.concatenate([jnp.broadcast_to(c[e:e + 1], (RB, TB)) == row for e in range(EL)], axis=0)


def spread(gate, b):
    g = gate[b]
    return jnp.concatenate([jnp.broadcast_to(g[e:e + 1], (RB, TB)) for e in range(EL)], axis=0)


def put_tables(b, code, gate, gs, tab):
    lane = lax.broadcasted_iota(jnp.int32, (EL, EL * RB), 1)
    widen = jnp.where(lane // RB == lax.broadcasted_iota(jnp.int32, (EL, EL * RB), 0), 1.0, 0.0).astype(BF)
    row = (lax.broadcasted_iota(jnp.int32, (TB, EL * RB), 1) % RB).astype(F32)
    sel = dot_tn(code[b].astype(F32).astype(BF), widen) == row
    g = gate[b]
    for i in range(3):
        part = g.astype(BF)
        g = g - part.astype(F32)
        tab[b, i] = jnp.where(sel, dot_tn(part, widen), 0.0).astype(BF)
    tab[b, 3] = jnp.where(sel, 1.0, 0.0).astype(BF)
    gs[b] = jnp.sum(jnp.where(select(code, b), spread(gate, b), 0.0), axis=1, keepdims=True)


def place(pos, core):
    y = pos // 4
    return pos + y * (7 - 2 * pos), 2 * y + core


def slot(pos, core):
    row, col = place(pos, core)
    return row * 4 + col


def remote(src, dst, ss, rs, dev):
    return pltpu.make_async_remote_copy(
        src_ref=src, dst_ref=dst, send_sem=ss, recv_sem=rs,
        device_id={'row': dev[0], 'col': dev[1]}, device_id_type=pl.DeviceIdType.MESH)


HALF = TOK // 2
NC = 4
CH = TOK // NC
LAST = 3 * NC + NC // 2
DH = D // 2


def main_kernel(ridx, gates, x, dy, w1h, w3h, w2h, yo, dxo, dgo, xrh, dorh, arh, durh, dvrh,
                w1, w3, w2, wsem, osem, isem, meta, xg, dyg, mg, code, gate, tab, xrow, orow, us, vs, av, gs, ds,
                acc, pbuf, rbuf, dgs, dgr,
                ags, agr, pgs, pgr, ms, mr, gss, gsr, rss, rsr, rps, rpr):
    z = lax.axis_index('row')
    c4 = lax.axis_index('col')
    yy = c4 // 2
    core = c4 % 2
    r = z + yy * (7 - 2 * z)
    me = z * 4 + c4
    base = me * EL
    right, left = (r + 1) % 8, (r + 7) % 8
    nbr = (place(right, core), place(left, core))
    partner = (z, 2 * yy + 1 - core)

    def peer(o):
        q = (me + o) % ND
        return q, (q // 4, q % 4)

    in_x = pltpu.make_async_copy(x, xg.at[me], isem.at[0])
    in_dy = pltpu.make_async_copy(dy, dyg.at[me], isem.at[1])
    in_x.start()
    in_dy.start()
    barrier = pltpu.get_barrier_semaphore()

    def hello(o, _):
        q, dev = peer(o)
        pl.semaphore_signal(barrier, inc=1, device_id={'row': dev[0], 'col': dev[1]},
                            device_id_type=pl.DeviceIdType.MESH)
        return 0

    lax.fori_loop(1, ND, hello, 0)

    def load(e, _):
        pltpu.make_async_copy(w1h.at[e], w1.at[e], wsem.at[e, 0]).start()
        pltpu.make_async_copy(w3h.at[e], w3.at[e], wsem.at[e, 1]).start()
        pltpu.make_async_copy(w2h.at[e], w2.at[e], wsem.at[e, 2]).start()
        return 0

    lax.fori_loop(0, EL, load, 0)
    both = jnp.concatenate([ridx[...].astype(F32), gates[...]], axis=0)
    both = jnp.concatenate([both, jnp.zeros((2 * TOP, 128 - TOK), F32)], axis=1)
    meta[...] = both
    mg[me] = both
    in_x.wait()
    in_dy.wait()
    pl.semaphore_wait(barrier, ND - 1)

    def meta_copy(o):
        q, dev = peer(o)
        return remote(meta, mg.at[me], ms.at[o], mr.at[o], dev)

    def meta_send(o, _):
        meta_copy(o).start()
        return 0

    def meta_wait(o, _):
        meta_copy(o).wait_recv()
        return 0

    lax.fori_loop(1, ND, meta_send, 0)

    gath = (xg, dyg)

    def own(t, d, m):
        h = m if d == 0 else NC - 1 - m
        c = gath[t].at[me, pl.ds(h * CH, CH)]
        return remote(c, c, ags.at[t, d, m], agr.at[t, d, m], nbr[d])

    def chunk(t, d, m):
        k = 1 + m // NC
        h = m % NC if d == 0 else NC - 1 - m % NC
        p = slot((r + 8 - k) % 8 if d == 0 else (r + k) % 8, core)
        return gath[t].at[p, pl.ds(pl.multiple_of(h * CH, CH), CH)]

    def onward(t, d, m):
        c = chunk(t, d, m)
        return remote(c, c, ags.at[t, d, m + NC], agr.at[t, d, m + NC], nbr[d])

    def across(t, d, m):
        c = chunk(t, d, m)
        return remote(c, c, pgs.at[t, d, m], pgr.at[t, d, m], partner)

    def own_across(t):
        c = gath[t].at[me]
        return remote(c, c, pgs.at[t, 0, LAST], pgr.at[t, 0, LAST], partner)

    def ag_start(t):
        for m in range(NC):
            for d in range(2):
                own(t, d, m).start()
        own_across(t).start()

    def ag_step(t, m):
        for d in range(2):
            c = chunk(t, d, m)
            remote(c, c, ags.at[t, d, m], agr.at[t, d, m], nbr[d]).wait_recv()

            @pl.when(m < LAST - NC)
            def _():
                onward(t, d, m).start()
            across(t, d, m).start()

    def ag_wait_partner(t):
        def body(m, _):
            for d in range(2):
                across(t, d, m).wait_recv()
            return 0
        lax.fori_loop(0, LAST, body, 0)
        own_across(t).wait_recv()

    def ag_drain(t):
        def body(m, _):
            for d in range(2):
                c = chunk(t, d, m)
                remote(c, c, ags.at[t, d, m], agr.at[t, d, m], nbr[d]).wait_send()
                across(t, d, m).wait_send()
            return 0
        lax.fori_loop(0, LAST, body, 0)
        own_across(t).wait_send()

    ag_start(0)

    def xstep(m, _):
        ag_step(0, m)

        @pl.when(m == 1)
        def _():
            lax.fori_loop(1, ND, meta_wait, 0)

        @pl.when((m >= 2) & (m < 10) & (m % 2 == 0))
        def _():
            put_codes(m // 2 - 1, base, mg, code, gate)

        @pl.when((m >= 3) & (m < 11) & (m % 2 == 1))
        def _():
            put_tables(m // 2 - 1, code, gate, gs, tab)
        return 0

    lax.fori_loop(0, LAST, xstep, 0)
    ag_start(1)
    ag_wait_partner(0)

    def gather(src, dst):
        def body(b, _):
            p = jnp.where(select(code, b), 1.0, 0.0).astype(BF)
            dst[b] = dot(p, src[pl.ds(NB * b, NB)].reshape(TB, D)).astype(BF)
            return 0
        lax.fori_loop(0, NB, body, 0)

    def rows_of(ref, e):
        return ref[:, pl.ds(pl.multiple_of(e * RB, RB), RB), :]

    def put_rows(ref, e, v):
        ref[:, pl.ds(pl.multiple_of(e * RB, RB), RB), :] = v.reshape(NB, RB, v.shape[-1])

    gather(xg, xrow)
    out_x = pltpu.make_async_copy(xrow, xrh, osem.at[0])
    out_x.start()

    def fwd(e, _):
        pltpu.make_async_copy(w1h.at[e], w1.at[e], wsem.at[e, 0]).wait()
        pltpu.make_async_copy(w3h.at[e], w3.at[e], wsem.at[e, 1]).wait()
        xe = rows_of(xrow, e).reshape(NB * RB, D)
        u = dot(xe, w1[e]).astype(BF)
        v = dot(xe, w3[e]).astype(BF)
        us[e] = u
        vs[e] = v
        uf = u.astype(F32)
        av[e] = (uf * jax.nn.sigmoid(uf) * v.astype(F32)).astype(BF)
        ag_step(1, e)
        return 0

    lax.fori_loop(0, EL, fwd, 0)
    out_a = pltpu.make_async_copy(av, arh, osem.at[1])
    out_a.start()

    def rs_pair(t, o):
        d = (r + o) % 8
        return remote(acc.at[t, slot(d, 1 - core)], pbuf.at[t, o], rps.at[t, o], rpr.at[t, o], partner)

    def rs_pair_block(t, b):
        for d in (b, 7 - b):
            rs_pair(t, (d + 8 - r) % 8).start()

    def rs_join(t, o):
        rs_pair(t, o).wait_recv()
        p = slot((r + o) % 8, core)
        acc[t, p] = acc[t, p] + pbuf[t, o]

    def rs_move(t, d, m):
        dist = 4 - (m + 1) // 2
        h = m % 2 if d == 0 else 1 - m % 2
        p = slot((r + dist) % 8 if d == 0 else (r + 8 - dist) % 8, core)
        rows = pl.ds(pl.multiple_of(h * HALF, HALF), HALF)
        return p, rows, remote(acc.at[t, p, rows], rbuf.at[t, d, m], rss.at[t, d, m], rsr.at[t, d, m], nbr[d])

    def rs_first(t):
        rs_join(t, 4)
        for d in range(2):
            rs_move(t, d, 0)[2].start()
        rs_join(t, 3)
        rs_join(t, 5)
        for d in range(2):
            rs_move(t, d, 1)[2].start()
        for o in (2, 6, 1, 7, 0):
            rs_join(t, o)

    def rs_step(t, m):
        for d in range(2):
            rs_move(t, d, m - 2)[2].wait_recv()
            p, rows, copy = rs_move(t, d, m)
            acc[t, p, rows] = acc[t, p, rows] + rbuf[t, d, m - 2]
            copy.start()

    def rs_last(t, out):
        cols = slice((t % 2) * DH, (t % 2) * DH + DH)
        for m in (5, 6):
            for d in range(2):
                rs_move(t, d, m)[2].wait_recv()
        out[:HALF, cols] = (acc[t, me, :HALF] + rbuf[t, 0, 6] + rbuf[t, 1, 5]).astype(BF)
        out[HALF:, cols] = (acc[t, me, HALF:] + rbuf[t, 0, 5] + rbuf[t, 1, 6]).astype(BF)

    def rs_drain(t):
        def body(m, _):
            for d in range(2):
                rs_move(t, d, m)[2].wait_send()
            return 0
        lax.fori_loop(0, 7, body, 0)

        def pair(o, _):
            rs_pair(t, o).wait_send()
            return 0
        lax.fori_loop(0, 8, pair, 0)

    def forward_half(c):
        cols = slice(c * DH, c * DH + DH)

        def out(e, _):
            if c == 0:
                pltpu.make_async_copy(w2h.at[e], w2.at[e], wsem.at[e, 2]).wait()
            orow[:, pl.ds(pl.multiple_of(e * RB, RB), RB), cols] = dot(av[e], w2[e, :, cols]).astype(BF).reshape(NB, RB, DH)
            return 0

        lax.fori_loop(0, EL, out, 0)

        def scatter(i, _):
            b = (3 - z + i) % NB
            o = orow[b, :, cols]
            acc[c, pl.ds(NB * b, NB)] = (dot(tab[b, 0], o) + dot(tab[b, 1], o) + dot(tab[b, 2], o)).reshape(NB, TOK, DH)
            rs_pair_block(c, b)
            if c == 0:
                @pl.when(i < 3)
                def _():
                    ag_step(1, EL + 2 * i)
                    ag_step(1, EL + 2 * i + 1)
            return 0

        lax.fori_loop(0, NB, scatter, 0)
        rs_first(c)

    forward_half(0)
    forward_half(1)
    rs_step(0, 2)
    ag_wait_partner(1)
    out_x.wait()
    gather(dyg, xrow)

    def bwd(e, _):
        dye = rows_of(xrow, e).reshape(NB * RB, D).astype(F32)
        o = rows_of(orow, e).reshape(NB * RB, D).astype(F32)
        put_rows(ds, e, jnp.sum(dye * o, axis=1, keepdims=True))
        g = rows_of(gs, e).reshape(NB * RB, 1)
        do = (g * dye).astype(BF)
        put_rows(xrow, e, do)
        da = dot_nt(do, w2[e])
        u = us[e].astype(F32)
        v = vs[e].astype(F32)
        s = jax.nn.sigmoid(u)
        du = (da * v * s * (1.0 + u * (1.0 - s))).astype(BF)
        dv = (da * u * s).astype(BF)
        us[e] = du
        vs[e] = dv
        put_rows(orow, e, (dot_nt(du, w1[e]) + dot_nt(dv, w3[e])).astype(BF))

        @pl.when(e < 7)
        def _():
            i = e + 1
            rs_step((i // 2) % 2, 2 + 2 * (i // 4) + i % 2)
        return 0

    lax.fori_loop(0, EL, bwd, 0)
    outs = [pltpu.make_async_copy(xrow, dorh, osem.at[2]), pltpu.make_async_copy(us, durh, osem.at[3]),
            pltpu.make_async_copy(vs, dvrh, osem.at[4])]
    for c in outs:
        c.start()
    rs_step(0, 6)

    def backward_half(c):
        cols = slice(c * DH, c * DH + DH)

        def scatter(i, _):
            b = (3 - z + i) % NB
            acc[2 + c, pl.ds(NB * b, NB)] = dot(tab[b, 3], orow[b, :, cols]).reshape(NB, TOK, DH)
            rs_pair_block(2 + c, b)
            return 0

        lax.fori_loop(0, NB, scatter, 0)
        rs_first(2 + c)

    backward_half(0)
    rs_step(1, 6)
    backward_half(1)

    def slots_back(b, _):
        dg = jnp.where(select(code, b), ds[b], 0.0)
        dge = jnp.concatenate([jnp.sum(dg[e * RB:(e + 1) * RB], axis=0, keepdims=True) for e in range(EL)], axis=0)
        for i in range(NB):
            dgs[NB * b + i, :, :TOK] = dge[:, i * TOK:(i + 1) * TOK]
        return 0

    lax.fori_loop(0, NB, slots_back, 0)

    def dg_copy(o):
        q, dev = peer(o)
        return remote(dgs.at[q], dgr.at[me], gss.at[o], gsr.at[o], dev)

    def dg_send(o, _):
        dg_copy(o).start()
        return 0

    lax.fori_loop(1, ND, dg_send, 0)
    dgr[me] = dgs[me]
    rs_step(2, 2)
    rs_step(2, 3)
    rs_step(3, 2)
    rs_last(0, yo)
    rs_step(3, 3)
    rs_last(1, yo)
    rs_step(2, 4)

    def dg_wait(o, _):
        dg_copy(o).wait_recv()
        return 0

    lax.fori_loop(1, ND, dg_wait, 0)
    rs_step(2, 5)
    expert = lax.broadcasted_iota(jnp.int32, (ND * EL, TOK), 0)
    back = dgr[...].reshape(ND * EL, 128)[:, :TOK]
    dgo[...] = jnp.concatenate(
        [jnp.sum(jnp.where(expert == ridx[j:j + 1], back, 0.0), axis=0, keepdims=True) for j in range(TOP)], axis=0)
    rs_step(3, 4)
    rs_step(3, 5)
    rs_step(2, 6)
    rs_step(3, 6)
    rs_last(2, dxo)
    rs_last(3, dxo)

    def small_drain(o, _):
        meta_copy(o).wait_send()
        dg_copy(o).wait_send()
        return 0

    lax.fori_loop(1, ND, small_drain, 0)
    for t in range(2):
        ag_drain(t)
    for t in range(4):
        rs_drain(t)
    out_a.wait()
    for c in outs:
        c.wait()


def main(ridx, gates, x, dy, w1, w3, w2):
    vm = pl.BlockSpec(memory_space=pltpu.VMEM)
    hb = pl.BlockSpec(memory_space=pl.ANY)
    sds = jax.ShapeDtypeStruct
    R = NB * RB
    dma = lambda *s: pltpu.SemaphoreType.DMA(s)
    return pl.pallas_call(
        main_kernel,
        out_shape=(sds((TOK, D), BF), sds((TOK, D), BF), sds((TOP, TOK), F32),
                   sds((NB, EL * RB, D), BF), sds((NB, EL * RB, D), BF), sds((EL, R, FF), BF), sds((EL, R, FF), BF), sds((EL, R, FF), BF)),
        in_specs=[vm, vm, hb, hb, hb, hb, hb],
        out_specs=[vm, vm, vm] + [hb] * 5,
        scratch_shapes=[
            pltpu.VMEM((EL, D, FF), BF), pltpu.VMEM((EL, D, FF), BF), pltpu.VMEM((EL, FF, D), BF),
            dma(EL, 3), dma(5), dma(2), pltpu.VMEM((2 * TOP, 128), F32),
            pltpu.VMEM((ND, TOK, D), BF), pltpu.VMEM((ND, TOK, D), BF), pltpu.VMEM((ND, 2 * TOP, 128), F32),
            pltpu.VMEM((NB, EL, TB), jnp.int32), pltpu.VMEM((NB, EL, TB), F32), pltpu.VMEM((NB, 4, TB, EL * RB), BF),
            pltpu.VMEM((NB, EL * RB, D), BF), pltpu.VMEM((NB, EL * RB, D), BF),
            pltpu.VMEM((EL, R, FF), BF), pltpu.VMEM((EL, R, FF), BF), pltpu.VMEM((EL, R, FF), BF),
            pltpu.VMEM((NB, EL * RB, 1), F32), pltpu.VMEM((NB, EL * RB, 1), F32),
            pltpu.VMEM((4, ND, TOK, DH), F32), pltpu.VMEM((4, 8, TOK, DH), F32), pltpu.VMEM((4, 2, 7, HALF, DH), F32),
            pltpu.VMEM((ND, EL, 128), F32), pltpu.VMEM((ND, EL, 128), F32),
            dma(2, 2, LAST), dma(2, 2, LAST), dma(2, 2, LAST + 1), dma(2, 2, LAST + 1), dma(ND), dma(ND), dma(ND), dma(ND),
            dma(4, 2, 7), dma(4, 2, 7), dma(4, 8), dma(4, 8),
        ],
        compiler_params=pltpu.CompilerParams(vmem_limit_bytes=VMEM_LIMIT, collective_id=0, has_side_effects=True),
        name='moe',
    )(ridx, gates, x, dy, w1, w3, w2)


def dw_kernel(y, dx, dg, x, do, a, du, dv, yo, dxo, dgo, g1, g3, g2):
    @pl.when(pl.program_id(0) == 0)
    def _():
        yo[...] = y[...]
        dxo[...] = dx[...]
        dgo[...] = dg[...]
    xb = x[...].reshape(NB * RB, D)
    g1[0] = dot_tn(xb, du[0])
    g3[0] = dot_tn(xb, dv[0])
    g2[0] = dot_tn(a[0], do[...].reshape(NB * RB, D))


def dw(y, dx, dg, xr, dor, ar, dur, dvr):
    sds = jax.ShapeDtypeStruct
    R = NB * RB
    whole = lambda *s: pl.BlockSpec(s, lambda e: (0, 0))
    act = pl.BlockSpec((1, R, FF), lambda e: (e, 0, 0))
    br = pl.BlockSpec((NB, RB, D), lambda e: (0, e, 0))
    same = [whole(TOK, D), whole(TOK, D), whole(TOP, TOK)]
    return pl.pallas_call(
        dw_kernel,
        grid=(EL,),
        out_shape=(sds((TOK, D), BF), sds((TOK, D), BF), sds((TOP, TOK), F32),
                   sds((EL, D, FF), F32), sds((EL, D, FF), F32), sds((EL, FF, D), F32)),
        in_specs=same + [br, br, act, act, act],
        out_specs=same + [pl.BlockSpec((1, D, FF), lambda e: (e, 0, 0)), pl.BlockSpec((1, D, FF), lambda e: (e, 0, 0)),
                          pl.BlockSpec((1, FF, D), lambda e: (e, 0, 0))],
        name='dw',
    )(y, dx, dg, xr, dor, ar, dur, dvr)


def solution(mesh):
    grp = ('row', 'col')
    tspec = P(('dp', 'row', 'col'), None)
    wspec = P(grp, None, None)
    gspec = P(('dp', 'row', 'col'), None, None)

    def local(x, ridx, gates, w1, w3, w2, dy):
        y, dx, dg, g1, g3, g2 = dw(*main(ridx.T, gates.T, x, dy, w1, w3, w2))
        return y, dx, dg.T, g1, g3, g2

    return jax.shard_map(local, mesh=mesh, in_specs=(tspec, tspec, tspec, wspec, wspec, wspec, tspec),
                         out_specs=(tspec, tspec, tspec, gspec, gspec, gspec), check_vma=False)
```

```python
import functools

import jax
import jax.numpy as jnp
from jax import lax
from jax.experimental import pallas as pl
from jax.experimental.pallas import tpu as pltpu
from jax.sharding import PartitionSpec as P

TOK = 64
ND = 16
D = 1024
FF = 384
EL = 8
TOP = 8
CAP = 16
NB = 4
TB = 4 * TOK
RB = 4 * CAP
NT = ND * TOK
BF = jnp.bfloat16
F32 = jnp.float32
VMEM_LIMIT = 67043328


def dot(a, b):
    return lax.dot_general(a, b, (((1,), (0,)), ((), ())), preferred_element_type=F32)


def dot_nt(a, b):
    return lax.dot_general(a, b, (((1,), (1,)), ((), ())), preferred_element_type=F32)


def dot_tn(a, b):
    return lax.dot_general(a, b, (((0,), (0,)), ((), ())), preferred_element_type=F32)


def put_codes(b, base, meta, code, gate):
    m = [meta[NB * b + i] for i in range(NB)]
    route = jnp.concatenate([a[:, :TOK] for a in m], axis=1)
    gates = jnp.concatenate([a[:, TOK:] for a in m], axis=1)
    rows, gr = [], []
    for e in range(EL):
        eq = route == (base + e).astype(F32)
        rows.append(jnp.sum(jnp.where(eq, 1.0, 0.0), axis=0, keepdims=True))
        gr.append(jnp.sum(jnp.where(eq, gates, 0.0), axis=0, keepdims=True))
    mem = jnp.concatenate(rows, axis=0)
    gate[b] = jnp.concatenate(gr, axis=0)
    i0 = lax.broadcasted_iota(jnp.int32, (TB, TB), 0)
    i1 = lax.broadcasted_iota(jnp.int32, (TB, TB), 1)
    upper = jnp.where((i0 < i1) & (i0 // TOK == i1 // TOK), 1.0, 0.0).astype(BF)
    src = lax.broadcasted_iota(jnp.int32, (EL, TB), 1) // TOK * CAP
    rank = dot(mem.astype(BF), upper).astype(jnp.int32)
    code[b] = jnp.where(mem > 0.5, rank + src, -1)


def select(code, b):
    row = lax.broadcasted_iota(jnp.int32, (RB, TB), 0)
    c = code[b]
    return jnp.concatenate([jnp.broadcast_to(c[e:e + 1], (RB, TB)) == row for e in range(EL)], axis=0)


def spread(gate, b):
    g = gate[b]
    return jnp.concatenate([jnp.broadcast_to(g[e:e + 1], (RB, TB)) for e in range(EL)], axis=0)


def put_tables(b, code, gate, gs, tab):
    lane = lax.broadcasted_iota(jnp.int32, (EL, EL * RB), 1)
    widen = jnp.where(lane // RB == lax.broadcasted_iota(jnp.int32, (EL, EL * RB), 0), 1.0, 0.0).astype(BF)
    row = (lax.broadcasted_iota(jnp.int32, (TB, EL * RB), 1) % RB).astype(F32)
    sel = dot_tn(code[b].astype(F32).astype(BF), widen) == row
    g = gate[b]
    for i in range(3):
        part = g.astype(BF)
        g = g - part.astype(F32)
        tab[b, i] = jnp.where(sel, dot_tn(part, widen), 0.0).astype(BF)
    tab[b, 3] = jnp.where(sel, 1.0, 0.0).astype(BF)
    gs[b] = jnp.sum(jnp.where(select(code, b), spread(gate, b), 0.0), axis=1, keepdims=True)


def place(pos, core):
    y = pos // 4
    return pos + y * (7 - 2 * pos), 2 * y + core


def remote(src, dst, ss, rs, dev):
    return pltpu.make_async_remote_copy(
        src_ref=src, dst_ref=dst, send_sem=ss, recv_sem=rs,
        device_id={'row': dev[0], 'col': dev[1]}, device_id_type=pl.DeviceIdType.MESH)


HALF = TOK // 2
NC = 4
CH = TOK // NC
LAST = 3 * NC + NC // 2
DH = D // 2
PEERS = [(o, k) for o in range(8) for k in range(2)][1:]


def main_kernel(ridx, gates, x, dy, w1h, w3h, w2h, yo, dxo, dgo, xrh, dorh, arh, durh, dvrh,
                w1, w3, w2, wsem, osem, isem, meta, xg, dyg, mg, code, gate, tab, xrow, orow, us, vs, av, gs, ds,
                acc, pbuf, rbuf, dgs, dgr,
                ags, agr, pgs, pgr, ms, mr, gss, gsr, rss, rsr, rps, rpr):
    z = lax.axis_index('row')
    c4 = lax.axis_index('col')
    yy = c4 // 2
    core = c4 % 2
    r = z + yy * (7 - 2 * z)
    base = (z * 4 + c4) * EL
    nbr = (place((r + 1) % 8, core), place((r + 7) % 8, core))
    partner = (z, 2 * yy + 1 - core)
    devs = [place((r + o) % 8, core if k == 0 else 1 - core) for o in range(8) for k in range(2)]

    in_x = pltpu.make_async_copy(x, xg.at[0], isem.at[0])
    in_dy = pltpu.make_async_copy(dy, dyg.at[0], isem.at[1])
    in_x.start()
    in_dy.start()
    barrier = pltpu.get_barrier_semaphore()
    for o, k in PEERS:
        dev = devs[2 * o + k]
        pl.semaphore_signal(barrier, inc=1, device_id={'row': dev[0], 'col': dev[1]},
                            device_id_type=pl.DeviceIdType.MESH)
    both = jnp.concatenate([ridx[...].astype(F32), gates[...]], axis=1)
    meta[...] = both
    mg[0] = both
    in_x.wait()
    in_dy.wait()
    pl.semaphore_wait(barrier, ND - 1)

    gath = (xg, dyg)

    def own(t, d, m):
        h = m if d == 0 else NC - 1 - m
        rows = slice(h * CH, h * CH + CH)
        return remote(gath[t].at[0, rows], gath[t].at[14 if d == 0 else 2, rows], ags.at[t, d, m], agr.at[t, d, m], nbr[d])

    def piece(d, m):
        k = 1 + lax.div(m, NC)
        h = lax.rem(m, NC) if d == 0 else NC - 1 - lax.rem(m, NC)
        return (8 - k) if d == 0 else k, pl.ds(pl.multiple_of(h * CH, CH), CH)

    def here(t, d, m):
        c = gath[t].at[0, :CH]
        return remote(c, c, ags.at[t, d, m], agr.at[t, d, m], nbr[d])

    def onward(t, d, m):
        o, rows = piece(d, m)
        return remote(gath[t].at[2 * o, rows], gath[t].at[2 * (o - 1 if d == 0 else o + 1), rows],
                      ags.at[t, d, m + NC], agr.at[t, d, m + NC], nbr[d])

    def across(t, d, m):
        o, rows = piece(d, m)
        return remote(gath[t].at[2 * o, rows], gath[t].at[2 * o + 1, rows], pgs.at[t, d, m], pgr.at[t, d, m], partner)

    def crossed(t, d, m):
        c = gath[t].at[0, :CH]
        return remote(c, c, pgs.at[t, d, m], pgr.at[t, d, m], partner)

    def own_across(t):
        return remote(gath[t].at[0], gath[t].at[1], pgs.at[t, 0, LAST], pgr.at[t, 0, LAST], partner)

    def ag_start(t):
        for m in range(NC):
            for d in range(2):
                own(t, d, m).start()
        own_across(t).start()

    def ag_step(t, m):
        for d in range(2):
            here(t, d, m).wait_recv()
            if isinstance(m, int):
                if m < LAST - NC:
                    onward(t, d, m).start()
            else:
                @pl.when(m < LAST - NC)
                def _():
                    onward(t, d, m).start()
            across(t, d, m).start()

    def ag_crossed(t, lo, hi):
        for m in range(lo, hi):
            for d in range(2):
                crossed(t, d, m).wait_recv()

    def meta_copy(o, k):
        return remote(meta, mg.at[2 * ((8 - o) % 8) + k], ms.at[2 * o + k], mr.at[2 * ((8 - o) % 8) + k], devs[2 * o + k])

    def meta_wait(o, k):
        return remote(meta, mg.at[0], ms.at[2 * o + k], mr.at[2 * o + k], devs[2 * o + k])

    for o, k in PEERS:
        meta_copy(o, k).start()
    ag_start(0)

    def gather_block(src, b):
        p = jnp.where(select(code, b), 1.0, 0.0).astype(BF)
        xrow[b] = dot(p, src[pl.ds(NB * b, NB)].reshape(TB, D)).astype(BF)

    def xload(m, _):
        ag_step(0, m)

        @pl.when(m > 0)
        def _():
            load13(m - 1)
        return 0

    def load13(e):
        pltpu.make_async_copy(w1h.at[e], w1.at[e], wsem.at[e, 0]).start()
        pltpu.make_async_copy(w3h.at[e], w3.at[e], wsem.at[e, 1]).start()

    lax.fori_loop(0, 3, xload, 0)
    for o, k in PEERS:
        meta_wait(o, k).wait_recv()

    def xstep(m, _):
        ag_step(0, m)
        load13(m - 1)

        @pl.when(m < 7)
        def _():
            put_codes(m - 3, base, mg, code, gate)

        @pl.when(m > 6)
        def _():
            put_tables(m - 7, code, gate, gs, tab)
        return 0

    lax.fori_loop(3, 9, xstep, 0)
    ag_step(0, 9)
    ag_start(1)
    put_tables(2, code, gate, gs, tab)
    ag_step(0, 10)
    ag_step(0, 11)
    for e in range(EL):
        pltpu.make_async_copy(w2h.at[e], w2.at[e], wsem.at[e, 2]).start()
    put_tables(3, code, gate, gs, tab)
    own_across(0).wait_recv()
    ag_crossed(0, 0, NC)
    gather_block(xg, 0)
    ag_step(0, 12)
    ag_crossed(0, NC, 2 * NC)
    gather_block(xg, 3)
    ag_step(0, 13)
    ag_crossed(0, 2 * NC, 3 * NC)
    gather_block(xg, 1)
    ag_step(1, 0)
    ag_step(1, 1)
    ag_crossed(0, 3 * NC, LAST)
    gather_block(xg, 2)
    ag_step(1, 2)
    ag_step(1, 3)

    def rows_of(ref, e):
        return ref[:, pl.ds(pl.multiple_of(e * RB, RB), RB), :]

    def put_rows(ref, e, v):
        ref[:, pl.ds(pl.multiple_of(e * RB, RB), RB), :] = v.reshape(NB, RB, v.shape[-1])

    out_x = pltpu.make_async_copy(xrow, xrh, osem.at[0])
    out_x.start()

    def fwd(e, _):
        pltpu.make_async_copy(w1h.at[e], w1.at[e], wsem.at[e, 0]).wait()
        pltpu.make_async_copy(w3h.at[e], w3.at[e], wsem.at[e, 1]).wait()
        xe = rows_of(xrow, e).reshape(NB * RB, D)
        u = dot(xe, w1[e]).astype(BF)
        v = dot(xe, w3[e]).astype(BF)
        us[e] = u
        vs[e] = v
        uf = u.astype(F32)
        av[e] = (uf * jax.nn.sigmoid(uf) * v.astype(F32)).astype(BF)
        ag_step(1, e + NC)
        return 0

    lax.fori_loop(0, EL, fwd, 0)
    out_a = pltpu.make_async_copy(av, arh, osem.at[1])
    out_a.start()

    def rs_pair(t, o):
        return remote(acc.at[t, 2 * o + 1], pbuf.at[t, o], rps.at[t, o], rpr.at[t, o], partner)

    def rs_join(t, o):
        rs_pair(t, o).wait_recv()
        acc[t, 2 * o] = acc[t, 2 * o] + pbuf[t, o]

    def rs_got(t, d, m):
        return remote(acc.at[0, 0, :HALF], rbuf.at[0, 0, 0], rss.at[t, d, m], rsr.at[t, d, m], nbr[d])

    def rs_move(t, d, m):
        dist = 4 - lax.div(m + 1, 2)
        h = lax.rem(m, 2) if d == 0 else 1 - lax.rem(m, 2)
        o = dist if d == 0 else 8 - dist
        rows = pl.ds(pl.multiple_of(h * HALF, HALF), HALF)
        return 2 * o, rows, remote(acc.at[t, 2 * o, rows], rbuf.at[t, d, m], rss.at[t, d, m], rsr.at[t, d, m], nbr[d])

    def rs_first(t):
        rs_join(t, 4)
        for d in range(2):
            rs_move(t, d, 0)[2].start()
        rs_join(t, 3)
        rs_join(t, 5)
        for d in range(2):
            rs_move(t, d, 1)[2].start()
        for o in (2, 6, 1, 7, 0):
            rs_join(t, o)

    def rs_step(t, m):
        for d in range(2):
            rs_got(t, d, m - 2).wait_recv()
            p, rows, copy = rs_move(t, d, m)
            acc[t, p, rows] = acc[t, p, rows] + rbuf[t, d, m - 2]
            copy.start()

    def rs_last(t, out):
        cols = slice((t % 2) * DH, (t % 2) * DH + DH)
        for m in (5, 6):
            for d in range(2):
                rs_got(t, d, m).wait_recv()
        out[:HALF, cols] = (acc[t, 0, :HALF] + rbuf[t, 0, 6] + rbuf[t, 1, 5]).astype(BF)
        out[HALF:, cols] = (acc[t, 0, HALF:] + rbuf[t, 0, 5] + rbuf[t, 1, 6]).astype(BF)

    def forward_half(c):
        cols = slice(c * DH, c * DH + DH)

        def out(e, _):
            if c == 0:
                pltpu.make_async_copy(w2h.at[e], w2.at[e], wsem.at[e, 2]).wait()
            orow[:, pl.ds(pl.multiple_of(e * RB, RB), RB), cols] = dot(av[e], w2[e, :, cols]).astype(BF).reshape(NB, RB, DH)
            return 0

        lax.fori_loop(0, EL, out, 0)
        if c == 0:
            ag_step(1, 12)
            ag_step(1, 13)

        def scatter(i, _):
            b = lax.rem(i + 2, NB)
            o = orow[b, :, cols]
            acc[c, pl.ds(NB * b, NB)] = (dot(tab[b, 0], o) + dot(tab[b, 1], o) + dot(tab[b, 2], o)).reshape(NB, TOK, DH)
            rs_pair(c, 2 * b).start()
            rs_pair(c, 2 * b + 1).start()
            if c == 1:
                for at, m in ((1, 2), (3, 3)):
                    @pl.when(i == at)
                    def _():
                        rs_step(0, m)
            return 0

        lax.fori_loop(0, NB, scatter, 0)
        rs_first(c)

    forward_half(0)
    forward_half(1)
    own_across(1).wait_recv()
    ag_crossed(1, 0, LAST)
    out_x.wait()

    def gather_dy(b, _):
        gather_block(dyg, b)
        return 0

    lax.fori_loop(0, NB, gather_dy, 0)
    rs_step(0, 4)

    def bwd(e, _):
        dye = rows_of(xrow, e).reshape(NB * RB, D).astype(F32)
        o = rows_of(orow, e).reshape(NB * RB, D).astype(F32)
        put_rows(ds, e, jnp.sum(dye * o, axis=1, keepdims=True))
        g = rows_of(gs, e).reshape(NB * RB, 1)
        do = (g * dye).astype(BF)
        put_rows(xrow, e, do)
        da = dot_nt(do, w2[e])
        u = us[e].astype(F32)
        v = vs[e].astype(F32)
        s = jax.nn.sigmoid(u)
        du = (da * v * s * (1.0 + u * (1.0 - s))).astype(BF)
        dv = (da * u * s).astype(BF)
        us[e] = du
        vs[e] = dv
        for at, t, m in ((1, 0, 5), (3, 1, 2), (5, 1, 3), (7, 0, 6)):
            @pl.when(e == at)
            def _():
                rs_step(t, m)
        return 0

    lax.fori_loop(0, EL, bwd, 0)
    outs = [pltpu.make_async_copy(xrow, dorh, osem.at[2]), pltpu.make_async_copy(us, durh, osem.at[3]),
            pltpu.make_async_copy(vs, dvrh, osem.at[4])]
    for c in outs:
        c.start()

    def slots_back(b, _):
        dg = jnp.where(select(code, b), ds[b], 0.0)
        dge = jnp.concatenate([jnp.sum(dg[e * RB:(e + 1) * RB], axis=0, keepdims=True) for e in range(EL)], axis=0)
        for i in range(NB):
            dgs[NB * b + i, :, :TOK] = dge[:, i * TOK:(i + 1) * TOK]
        return 0

    lax.fori_loop(0, NB, slots_back, 0)

    def dg_copy(o, k):
        return remote(dgs.at[2 * o + k], dgr.at[2 * ((8 - o) % 8) + k], gss.at[2 * o + k], gsr.at[2 * ((8 - o) % 8) + k],
                      devs[2 * o + k])

    def dg_wait(o, k):
        return remote(dgs.at[0], dgr.at[0], gss.at[2 * o + k], gsr.at[2 * o + k], devs[2 * o + k])

    for o, k in PEERS:
        dg_copy(o, k).start()
    dgr[0] = dgs[0]

    def backward_half(c):
        cols = slice(c * DH, c * DH + DH)

        def back(e, _):
            dx = dot_nt(us[e], w1[e, cols, :]) + dot_nt(vs[e], w3[e, cols, :])
            orow[:, pl.ds(pl.multiple_of(e * RB, RB), RB), cols] = dx.astype(BF).reshape(NB, RB, DH)
            if c == 0:
                for at, m in ((3, 4), (7, 5)):
                    @pl.when(e == at)
                    def _():
                        rs_step(1, m)
            return 0

        lax.fori_loop(0, EL, back, 0)

        def scatter(i, _):
            b = lax.rem(i + 2, NB)
            acc[2 + c, pl.ds(NB * b, NB)] = dot(tab[b, 3], orow[b, :, cols]).reshape(NB, TOK, DH)
            rs_pair(2 + c, 2 * b).start()
            rs_pair(2 + c, 2 * b + 1).start()
            return 0

        lax.fori_loop(0, NB, scatter, 0)
        rs_first(2 + c)

    backward_half(0)
    rs_step(1, 6)
    backward_half(1)

    rs_step(2, 2)
    rs_step(2, 3)
    rs_step(3, 2)
    rs_last(0, yo)
    rs_step(3, 3)
    rs_last(1, yo)
    rs_step(2, 4)
    rs_step(2, 5)
    rs_step(3, 4)
    rs_step(3, 5)
    for o, k in PEERS:
        dg_wait(o, k).wait_recv()
    lane = lax.broadcasted_iota(jnp.int32, (EL, TOK), 0)
    total = [jnp.zeros((EL, TOK), F32)] * TOP
    for i in range(ND):
        expert = lane + (devs[i][0] * 4 + devs[i][1]) * EL
        back = dgr[i, :, :TOK]
        total = [t + jnp.where(expert == ridx[j:j + 1], back, 0.0) for j, t in enumerate(total)]
    dgo[...] = jnp.concatenate([jnp.sum(t, axis=0, keepdims=True) for t in total], axis=0)
    for t in range(2):
        own_across(t).wait_send()
        for m in range(LAST):
            for d in range(2):
                here(t, d, m).wait_send()
                crossed(t, d, m).wait_send()
    for o, k in PEERS:
        meta_wait(o, k).wait_send()
        dg_wait(o, k).wait_send()
    out_a.wait()
    rs_step(2, 6)
    for c in outs:
        c.wait()
    for t in range(4):
        for o in range(8):
            rs_pair(t, o).wait_send()
    rs_step(3, 6)
    for t in range(2):
        for m in range(7):
            for d in range(2):
                rs_got(t, d, m).wait_send()
    rs_last(2, dxo)
    rs_last(3, dxo)
    for t in range(2, 4):
        for m in range(7):
            for d in range(2):
                rs_got(t, d, m).wait_send()


def main(ridx, gates, x, dy, w1, w3, w2):
    vm = pl.BlockSpec(memory_space=pltpu.VMEM)
    hb = pl.BlockSpec(memory_space=pl.ANY)
    sds = jax.ShapeDtypeStruct
    R = NB * RB
    dma = lambda *s: pltpu.SemaphoreType.DMA(s)
    return pl.pallas_call(
        main_kernel,
        out_shape=(sds((TOK, D), BF), sds((TOK, D), BF), sds((TOP, TOK), F32),
                   sds((NB, EL * RB, D), BF), sds((NB, EL * RB, D), BF), sds((EL, R, FF), BF), sds((EL, R, FF), BF), sds((EL, R, FF), BF)),
        in_specs=[vm, vm, hb, hb, hb, hb, hb],
        out_specs=[vm, vm, vm] + [hb] * 5,
        scratch_shapes=[
            pltpu.VMEM((EL, D, FF), BF), pltpu.VMEM((EL, D, FF), BF), pltpu.VMEM((EL, FF, D), BF),
            dma(EL, 3), dma(5), dma(2), pltpu.VMEM((TOP, 128), F32),
            pltpu.VMEM((ND, TOK, D), BF), pltpu.VMEM((ND, TOK, D), BF), pltpu.VMEM((ND, TOP, 128), F32),
            pltpu.VMEM((NB, EL, TB), jnp.int32), pltpu.VMEM((NB, EL, TB), F32), pltpu.VMEM((NB, 4, TB, EL * RB), BF),
            pltpu.VMEM((NB, EL * RB, D), BF), pltpu.VMEM((NB, EL * RB, D), BF),
            pltpu.VMEM((EL, R, FF), BF), pltpu.VMEM((EL, R, FF), BF), pltpu.VMEM((EL, R, FF), BF),
            pltpu.VMEM((NB, EL * RB, 1), F32), pltpu.VMEM((NB, EL * RB, 1), F32),
            pltpu.VMEM((4, ND, TOK, DH), F32), pltpu.VMEM((4, 8, TOK, DH), F32), pltpu.VMEM((4, 2, 7, HALF, DH), F32),
            pltpu.VMEM((ND, EL, 128), F32), pltpu.VMEM((ND, EL, 128), F32),
            dma(2, 2, LAST), dma(2, 2, LAST), dma(2, 2, LAST + 1), dma(2, 2, LAST + 1), dma(ND), dma(ND), dma(ND), dma(ND),
            dma(4, 2, 7), dma(4, 2, 7), dma(4, 8), dma(4, 8),
        ],
        compiler_params=pltpu.CompilerParams(vmem_limit_bytes=VMEM_LIMIT, collective_id=0, has_side_effects=True),
        name='moe',
    )(ridx, gates, x, dy, w1, w3, w2)


def dw_kernel(y, dx, dg, x, do, a, du, dv, yo, dxo, dgo, g1, g3, g2):
    @pl.when(pl.program_id(0) == 0)
    def _():
        yo[...] = y[...]
        dxo[...] = dx[...]
        dgo[...] = dg[...]
    xb = x[...].reshape(NB * RB, D)
    g1[0] = dot_tn(xb, du[0])
    g3[0] = dot_tn(xb, dv[0])
    g2[0] = dot_tn(a[0], do[...].reshape(NB * RB, D))


def dw(y, dx, dg, xr, dor, ar, dur, dvr):
    sds = jax.ShapeDtypeStruct
    R = NB * RB
    whole = lambda *s: pl.BlockSpec(s, lambda e: (0, 0))
    act = pl.BlockSpec((1, R, FF), lambda e: (e, 0, 0))
    br = pl.BlockSpec((NB, RB, D), lambda e: (0, e, 0))
    same = [whole(TOK, D), whole(TOK, D), whole(TOP, TOK)]
    return pl.pallas_call(
        dw_kernel,
        grid=(EL,),
        out_shape=(sds((TOK, D), BF), sds((TOK, D), BF), sds((TOP, TOK), F32),
                   sds((EL, D, FF), F32), sds((EL, D, FF), F32), sds((EL, FF, D), F32)),
        in_specs=same + [br, br, act, act, act],
        out_specs=same + [pl.BlockSpec((1, D, FF), lambda e: (e, 0, 0)), pl.BlockSpec((1, D, FF), lambda e: (e, 0, 0)),
                          pl.BlockSpec((1, FF, D), lambda e: (e, 0, 0))],
        name='dw',
    )(y, dx, dg, xr, dor, ar, dur, dvr)


def solution(mesh):
    grp = ('row', 'col')
    tspec = P(('dp', 'row', 'col'), None)
    wspec = P(grp, None, None)
    gspec = P(('dp', 'row', 'col'), None, None)

    def local(x, ridx, gates, w1, w3, w2, dy):
        y, dx, dg, g1, g3, g2 = dw(*main(ridx.T, gates.T, x, dy, w1, w3, w2))
        return y, dx, dg.T, g1, g3, g2

    return jax.shard_map(local, mesh=mesh, in_specs=(tspec, tspec, tspec, wspec, wspec, wspec, tspec),
                         out_specs=(tspec, tspec, tspec, gspec, gspec, gspec), check_vma=False)
```

```python
import functools

import jax
import jax.numpy as jnp
from jax import lax
from jax.experimental import pallas as pl
from jax.experimental.pallas import tpu as pltpu
from jax.sharding import PartitionSpec as P

TOK = 64
ND = 16
D = 1024
FF = 384
EL = 8
TOP = 8
CAP = 16
NB = 4
TB = 4 * TOK
RB = 4 * CAP
NT = ND * TOK
BF = jnp.bfloat16
F32 = jnp.float32
VMEM_LIMIT = 67043328


def dot(a, b):
    return lax.dot_general(a, b, (((1,), (0,)), ((), ())), preferred_element_type=F32)


def dot_nt(a, b):
    return lax.dot_general(a, b, (((1,), (1,)), ((), ())), preferred_element_type=F32)


def dot_tn(a, b):
    return lax.dot_general(a, b, (((0,), (0,)), ((), ())), preferred_element_type=F32)


def put_codes(b, base, meta, code, gate):
    m = [meta[NB * b + i] for i in range(NB)]
    route = jnp.concatenate([a[:, :TOK] for a in m], axis=1)
    gates = jnp.concatenate([a[:, TOK:] for a in m], axis=1)
    rows, gr = [], []
    for e in range(EL):
        eq = route == (base + e).astype(F32)
        rows.append(jnp.sum(jnp.where(eq, 1.0, 0.0), axis=0, keepdims=True))
        gr.append(jnp.sum(jnp.where(eq, gates, 0.0), axis=0, keepdims=True))
    mem = jnp.concatenate(rows, axis=0)
    gate[b] = jnp.concatenate(gr, axis=0)
    i0 = lax.broadcasted_iota(jnp.int32, (TB, TB), 0)
    i1 = lax.broadcasted_iota(jnp.int32, (TB, TB), 1)
    upper = jnp.where((i0 < i1) & (i0 // TOK == i1 // TOK), 1.0, 0.0).astype(BF)
    src = lax.broadcasted_iota(jnp.int32, (EL, TB), 1) // TOK * CAP
    rank = dot(mem.astype(BF), upper).astype(jnp.int32)
    code[b] = jnp.where(mem > 0.5, rank + src, -1)


def select(code, b):
    row = lax.broadcasted_iota(jnp.int32, (RB, TB), 0)
    c = code[b]
    return jnp.concatenate([jnp.broadcast_to(c[e:e + 1], (RB, TB)) == row for e in range(EL)], axis=0)


def spread(gate, b):
    g = gate[b]
    return jnp.concatenate([jnp.broadcast_to(g[e:e + 1], (RB, TB)) for e in range(EL)], axis=0)


def put_tables(b, code, gate, gs, tab):
    lane = lax.broadcasted_iota(jnp.int32, (EL, EL * RB), 1)
    widen = jnp.where(lane // RB == lax.broadcasted_iota(jnp.int32, (EL, EL * RB), 0), 1.0, 0.0).astype(BF)
    row = (lax.broadcasted_iota(jnp.int32, (TB, EL * RB), 1) % RB).astype(F32)
    sel = dot_tn(code[b].astype(F32).astype(BF), widen) == row
    g = gate[b]
    for i in range(3):
        part = g.astype(BF)
        g = g - part.astype(F32)
        tab[b, i] = jnp.where(sel, dot_tn(part, widen), 0.0).astype(BF)
    tab[b, 3] = jnp.where(sel, 1.0, 0.0).astype(BF)
    gs[b] = jnp.sum(jnp.where(select(code, b), spread(gate, b), 0.0), axis=1, keepdims=True)


def place(pos, core):
    y = pos // 4
    return pos + y * (7 - 2 * pos), 2 * y + core


def remote(src, dst, ss, rs, dev):
    return pltpu.make_async_remote_copy(
        src_ref=src, dst_ref=dst, send_sem=ss, recv_sem=rs,
        device_id={'row': dev[0], 'col': dev[1]}, device_id_type=pl.DeviceIdType.MESH)


HALF = TOK // 2
NC = 4
CH = TOK // NC
LAST = 3 * NC + NC // 2
DH = D // 2
PEERS = [(o, k) for o in range(8) for k in range(2)][1:]


def main_kernel(ridxh, gatesh, x, dy, w1h, w3h, w2h, yo, dxo, dgo, xrh, dorh, arh, durh, dvrh,
                w1, w3, w2, wsem, osem, isem, ridx, gates, meta, xg, dyg, mg, code, gate, tab, xrow, orow, us, vs, av, gs, ds,
                acc, pbuf, rbuf, dgs, dgr,
                ags, agr, pgs, pgr, ms, mr, gss, gsr, rss, rsr, rps, rpr):
    z = lax.axis_index('row')
    c4 = lax.axis_index('col')
    yy = c4 // 2
    core = c4 % 2
    r = z + yy * (7 - 2 * z)
    base = (z * 4 + c4) * EL
    nbr = (place((r + 1) % 8, core), place((r + 7) % 8, core))
    partner = (z, 2 * yy + 1 - core)
    devs = [place((r + o) % 8, core if k == 0 else 1 - core) for o in range(8) for k in range(2)]

    in_x = pltpu.make_async_copy(x, xg.at[0], isem.at[0])
    in_dy = pltpu.make_async_copy(dy, dyg.at[0], isem.at[1])
    in_r = pltpu.make_async_copy(ridxh, ridx, isem.at[2])
    in_g = pltpu.make_async_copy(gatesh, gates, isem.at[3])
    in_r.start()
    in_g.start()
    in_x.start()
    in_dy.start()
    barrier = pltpu.get_barrier_semaphore()
    for o, k in PEERS:
        dev = devs[2 * o + k]
        pl.semaphore_signal(barrier, inc=1, device_id={'row': dev[0], 'col': dev[1]},
                            device_id_type=pl.DeviceIdType.MESH)
    in_r.wait()
    in_g.wait()
    both = jnp.concatenate([ridx[...].astype(F32), gates[...]], axis=1)
    meta[...] = both
    mg[0] = both
    in_x.wait()
    in_dy.wait()
    pl.semaphore_wait(barrier, ND - 1)

    gath = (xg, dyg)

    def own(t, d, m):
        h = m if d == 0 else NC - 1 - m
        rows = slice(h * CH, h * CH + CH)
        return remote(gath[t].at[0, rows], gath[t].at[14 if d == 0 else 2, rows], ags.at[t, d, m], agr.at[t, d, m], nbr[d])

    def piece(d, m):
        k = 1 + lax.div(m, NC)
        h = lax.rem(m, NC) if d == 0 else NC - 1 - lax.rem(m, NC)
        return (8 - k) if d == 0 else k, pl.ds(pl.multiple_of(h * CH, CH), CH)

    def here(t, d, m):
        c = gath[t].at[0, :CH]
        return remote(c, c, ags.at[t, d, m], agr.at[t, d, m], nbr[d])

    def onward(t, d, m):
        o, rows = piece(d, m)
        return remote(gath[t].at[2 * o, rows], gath[t].at[2 * (o - 1 if d == 0 else o + 1), rows],
                      ags.at[t, d, m + NC], agr.at[t, d, m + NC], nbr[d])

    def across(t, d, m):
        o, rows = piece(d, m)
        return remote(gath[t].at[2 * o, rows], gath[t].at[2 * o + 1, rows], pgs.at[t, d, m], pgr.at[t, d, m], partner)

    def crossed(t, d, m):
        c = gath[t].at[0, :CH]
        return remote(c, c, pgs.at[t, d, m], pgr.at[t, d, m], partner)

    def own_across(t):
        return remote(gath[t].at[0], gath[t].at[1], pgs.at[t, 0, LAST], pgr.at[t, 0, LAST], partner)

    def ag_start(t):
        for m in range(NC):
            for d in range(2):
                own(t, d, m).start()
        own_across(t).start()

    def ag_step(t, m):
        for d in range(2):
            here(t, d, m).wait_recv()
            if isinstance(m, int):
                if m < LAST - NC:
                    onward(t, d, m).start()
            else:
                @pl.when(m < LAST - NC)
                def _():
                    onward(t, d, m).start()
            across(t, d, m).start()

    def ag_crossed(t, lo, hi):
        for m in range(lo, hi):
            for d in range(2):
                crossed(t, d, m).wait_recv()

    def meta_copy(o, k):
        return remote(meta, mg.at[2 * ((8 - o) % 8) + k], ms.at[2 * o + k], mr.at[2 * ((8 - o) % 8) + k], devs[2 * o + k])

    def meta_wait(o, k):
        return remote(meta, mg.at[0], ms.at[2 * o + k], mr.at[2 * o + k], devs[2 * o + k])

    for o, k in PEERS:
        meta_copy(o, k).start()
    ag_start(0)

    def gather_block(src, b):
        p = jnp.where(select(code, b), 1.0, 0.0).astype(BF)
        xrow[b] = dot(p, src[pl.ds(NB * b, NB)].reshape(TB, D)).astype(BF)

    def xload(m, _):
        ag_step(0, m)

        @pl.when(m > 0)
        def _():
            load13(m - 1)
        return 0

    def load13(e):
        pltpu.make_async_copy(w1h.at[e], w1.at[e], wsem.at[e, 0]).start()
        pltpu.make_async_copy(w3h.at[e], w3.at[e], wsem.at[e, 1]).start()

    lax.fori_loop(0, 5, xload, 0)
    for o, k in PEERS:
        meta_wait(o, k).wait_recv()

    def xstep(m, _):
        ag_step(0, m)
        load13(m - 1)

        put_codes(m - 5, base, mg, code, gate)
        return 0

    lax.fori_loop(5, 9, xstep, 0)
    ag_step(0, 9)
    ag_start(1)
    put_tables(0, code, gate, gs, tab)
    ag_step(0, 10)
    for e in range(EL):
        pltpu.make_async_copy(w2h.at[e], w2.at[e], wsem.at[e, 2]).start()
    put_tables(1, code, gate, gs, tab)
    ag_step(0, 11)
    put_tables(2, code, gate, gs, tab)
    put_tables(3, code, gate, gs, tab)
    own_across(0).wait_recv()
    ag_crossed(0, 0, NC)
    gather_block(xg, 0)
    ag_step(0, 12)
    ag_crossed(0, NC, 2 * NC)
    gather_block(xg, 3)
    ag_step(0, 13)
    ag_crossed(0, 2 * NC, 3 * NC)
    gather_block(xg, 1)
    ag_step(1, 0)
    ag_step(1, 1)
    ag_crossed(0, 3 * NC, LAST)
    gather_block(xg, 2)
    ag_step(1, 2)
    ag_step(1, 3)

    def rows_of(ref, e):
        return ref[:, pl.ds(pl.multiple_of(e * RB, RB), RB), :]

    def put_rows(ref, e, v):
        ref[:, pl.ds(pl.multiple_of(e * RB, RB), RB), :] = v.reshape(NB, RB, v.shape[-1])

    out_x = pltpu.make_async_copy(xrow, xrh, osem.at[0])
    out_x.start()

    def fwd(e, _):
        pltpu.make_async_copy(w1h.at[e], w1.at[e], wsem.at[e, 0]).wait()
        pltpu.make_async_copy(w3h.at[e], w3.at[e], wsem.at[e, 1]).wait()
        xe = rows_of(xrow, e).reshape(NB * RB, D)
        u = dot(xe, w1[e]).astype(BF)
        v = dot(xe, w3[e]).astype(BF)
        us[e] = u
        vs[e] = v
        uf = u.astype(F32)
        av[e] = (uf * jax.nn.sigmoid(uf) * v.astype(F32)).astype(BF)
        ag_step(1, e + NC)
        return 0

    lax.fori_loop(0, EL, fwd, 0)
    out_a = pltpu.make_async_copy(av, arh, osem.at[1])
    out_a.start()

    def rs_pair(t, o):
        return remote(acc.at[t, 2 * o + 1], pbuf.at[t, o], rps.at[t, o], rpr.at[t, o], partner)

    def rs_join(t, o):
        rs_pair(t, o).wait_recv()
        acc[t, 2 * o] = acc[t, 2 * o] + pbuf[t, o]

    def rs_got(t, d, m):
        return remote(acc.at[0, 0, :HALF], rbuf.at[0, 0, 0], rss.at[t, d, m], rsr.at[t, d, m], nbr[d])

    def rs_move(t, d, m):
        dist = 4 - lax.div(m + 1, 2)
        h = lax.rem(m, 2) if d == 0 else 1 - lax.rem(m, 2)
        o = dist if d == 0 else 8 - dist
        rows = pl.ds(pl.multiple_of(h * HALF, HALF), HALF)
        return 2 * o, rows, remote(acc.at[t, 2 * o, rows], rbuf.at[t, d, m], rss.at[t, d, m], rsr.at[t, d, m], nbr[d])

    def rs_first(t):
        rs_join(t, 4)
        for d in range(2):
            rs_move(t, d, 0)[2].start()
        rs_join(t, 3)
        rs_join(t, 5)
        for d in range(2):
            rs_move(t, d, 1)[2].start()
        for o in (2, 6, 1, 7, 0):
            rs_join(t, o)

    def rs_step(t, m):
        for d in range(2):
            rs_got(t, d, m - 2).wait_recv()
            p, rows, copy = rs_move(t, d, m)
            acc[t, p, rows] = acc[t, p, rows] + rbuf[t, d, m - 2]
            copy.start()

    def rs_last(t, out):
        cols = slice((t % 2) * DH, (t % 2) * DH + DH)
        for m in (5, 6):
            for d in range(2):
                rs_got(t, d, m).wait_recv()
        out[:HALF, cols] = (acc[t, 0, :HALF] + rbuf[t, 0, 6] + rbuf[t, 1, 5]).astype(BF)
        out[HALF:, cols] = (acc[t, 0, HALF:] + rbuf[t, 0, 5] + rbuf[t, 1, 6]).astype(BF)

    def forward_half(c):
        cols = slice(c * DH, c * DH + DH)

        def out(e, _):
            if c == 0:
                pltpu.make_async_copy(w2h.at[e], w2.at[e], wsem.at[e, 2]).wait()
            orow[:, pl.ds(pl.multiple_of(e * RB, RB), RB), cols] = dot(av[e], w2[e, :, cols]).astype(BF).reshape(NB, RB, DH)
            return 0

        lax.fori_loop(0, EL, out, 0)
        if c == 0:
            ag_step(1, 12)
            ag_step(1, 13)

        def scatter(i, _):
            b = lax.rem(i + 2, NB)
            o = orow[b, :, cols]
            acc[c, pl.ds(NB * b, NB)] = (dot(tab[b, 0], o) + dot(tab[b, 1], o) + dot(tab[b, 2], o)).reshape(NB, TOK, DH)
            rs_pair(c, 2 * b).start()
            rs_pair(c, 2 * b + 1).start()
            if c == 1:
                for at, m in ((1, 2), (3, 3)):
                    @pl.when(i == at)
                    def _():
                        rs_step(0, m)
            return 0

        lax.fori_loop(0, NB, scatter, 0)
        rs_first(c)

    forward_half(0)
    forward_half(1)
    own_across(1).wait_recv()
    ag_crossed(1, 0, LAST)
    out_x.wait()

    def gather_dy(b, _):
        gather_block(dyg, b)
        return 0

    lax.fori_loop(0, NB, gather_dy, 0)
    rs_step(0, 4)

    def bwd(e, _):
        dye = rows_of(xrow, e).reshape(NB * RB, D).astype(F32)
        o = rows_of(orow, e).reshape(NB * RB, D).astype(F32)
        put_rows(ds, e, jnp.sum(dye * o, axis=1, keepdims=True))
        g = rows_of(gs, e).reshape(NB * RB, 1)
        do = (g * dye).astype(BF)
        put_rows(xrow, e, do)
        da = dot_nt(do, w2[e])
        u = us[e].astype(F32)
        v = vs[e].astype(F32)
        s = jax.nn.sigmoid(u)
        du = (da * v * s * (1.0 + u * (1.0 - s))).astype(BF)
        dv = (da * u * s).astype(BF)
        us[e] = du
        vs[e] = dv
        for at, t, m in ((1, 0, 5), (3, 1, 2), (5, 1, 3), (7, 0, 6)):
            @pl.when(e == at)
            def _():
                rs_step(t, m)
        return 0

    lax.fori_loop(0, EL, bwd, 0)
    outs = [pltpu.make_async_copy(xrow, dorh, osem.at[2]), pltpu.make_async_copy(us, durh, osem.at[3]),
            pltpu.make_async_copy(vs, dvrh, osem.at[4])]
    for c in outs:
        c.start()

    def slots_back(b, _):
        dg = jnp.where(select(code, b), ds[b], 0.0)
        dge = jnp.concatenate([jnp.sum(dg[e * RB:(e + 1) * RB], axis=0, keepdims=True) for e in range(EL)], axis=0)
        for i in range(NB):
            dgs[NB * b + i, :, :TOK] = dge[:, i * TOK:(i + 1) * TOK]
        return 0

    lax.fori_loop(0, NB, slots_back, 0)

    def dg_copy(o, k):
        return remote(dgs.at[2 * o + k], dgr.at[2 * ((8 - o) % 8) + k], gss.at[2 * o + k], gsr.at[2 * ((8 - o) % 8) + k],
                      devs[2 * o + k])

    def dg_wait(o, k):
        return remote(dgs.at[0], dgr.at[0], gss.at[2 * o + k], gsr.at[2 * o + k], devs[2 * o + k])

    for o, k in PEERS:
        dg_copy(o, k).start()
    dgr[0] = dgs[0]


    def backward_half(c):
        cols = slice(c * DH, c * DH + DH)

        def back(e, _):
            dx = dot_nt(us[e], w1[e, cols, :]) + dot_nt(vs[e], w3[e, cols, :])
            orow[:, pl.ds(pl.multiple_of(e * RB, RB), RB), cols] = dx.astype(BF).reshape(NB, RB, DH)
            if c == 0:
                for at, m in ((3, 4), (7, 5)):
                    @pl.when(e == at)
                    def _():
                        rs_step(1, m)
            else:
                @pl.when(e == 7)
                def _():
                    rs_step(2, 2)
            return 0

        lax.fori_loop(0, EL, back, 0)

        def scatter(i, _):
            b = lax.rem(i + 2, NB)
            acc[2 + c, pl.ds(NB * b, NB)] = dot(tab[b, 3], orow[b, :, cols]).reshape(NB, TOK, DH)
            rs_pair(2 + c, 2 * b).start()
            rs_pair(2 + c, 2 * b + 1).start()
            if c == 1:
                @pl.when(i == 2)
                def _():
                    rs_step(2, 3)
            return 0

        lax.fori_loop(0, NB, scatter, 0)
        rs_first(2 + c)

    backward_half(0)
    rs_step(1, 6)
    backward_half(1)

    rs_last(0, yo)
    rs_step(2, 4)
    rs_last(1, yo)
    rs_step(2, 5)
    rs_step(3, 2)
    rs_step(3, 3)
    rs_step(2, 6)
    rs_step(3, 4)
    rs_step(3, 5)
    for t in range(2):
        own_across(t).wait_send()
        for m in range(LAST):
            for d in range(2):
                here(t, d, m).wait_send()
                crossed(t, d, m).wait_send()
    for o, k in PEERS:
        meta_wait(o, k).wait_send()
    out_a.wait()
    for c in outs:
        c.wait()
    for t in range(4):
        for o in range(8):
            rs_pair(t, o).wait_send()
    rs_step(3, 6)
    for t in range(2):
        for m in range(7):
            for d in range(2):
                rs_got(t, d, m).wait_send()
    rs_last(2, dxo)
    rs_last(3, dxo)
    for o, k in PEERS:
        dg_wait(o, k).wait_recv()
    lane = lax.broadcasted_iota(jnp.int32, (EL, TOK), 0)
    total = [jnp.zeros((EL, TOK), F32)] * TOP
    for i in range(ND):
        expert = lane + (devs[i][0] * 4 + devs[i][1]) * EL
        back = dgr[i, :, :TOK]
        total = [t + jnp.where(expert == ridx[j:j + 1], back, 0.0) for j, t in enumerate(total)]
    dgo[...] = jnp.concatenate([jnp.sum(t, axis=0, keepdims=True) for t in total], axis=0)
    for o, k in PEERS:
        dg_wait(o, k).wait_send()
    for t in range(2, 4):
        for m in range(7):
            for d in range(2):
                rs_got(t, d, m).wait_send()


def main(ridx, gates, x, dy, w1, w3, w2):
    vm = pl.BlockSpec(memory_space=pltpu.VMEM)
    hb = pl.BlockSpec(memory_space=pl.ANY)
    sds = jax.ShapeDtypeStruct
    R = NB * RB
    dma = lambda *s: pltpu.SemaphoreType.DMA(s)
    return pl.pallas_call(
        main_kernel,
        out_shape=(sds((TOK, D), BF), sds((TOK, D), BF), sds((TOP, TOK), F32),
                   sds((NB, EL * RB, D), BF), sds((NB, EL * RB, D), BF), sds((EL, R, FF), BF), sds((EL, R, FF), BF), sds((EL, R, FF), BF)),
        in_specs=[hb] * 7,
        out_specs=[vm, vm, vm] + [hb] * 5,
        scratch_shapes=[
            pltpu.VMEM((EL, D, FF), BF), pltpu.VMEM((EL, D, FF), BF), pltpu.VMEM((EL, FF, D), BF),
            dma(EL, 3), dma(5), dma(4), pltpu.VMEM((TOP, TOK), jnp.int32), pltpu.VMEM((TOP, TOK), F32), pltpu.VMEM((TOP, 128), F32),
            pltpu.VMEM((ND, TOK, D), BF), pltpu.VMEM((ND, TOK, D), BF), pltpu.VMEM((ND, TOP, 128), F32),
            pltpu.VMEM((NB, EL, TB), jnp.int32), pltpu.VMEM((NB, EL, TB), F32), pltpu.VMEM((NB, 4, TB, EL * RB), BF),
            pltpu.VMEM((NB, EL * RB, D), BF), pltpu.VMEM((NB, EL * RB, D), BF),
            pltpu.VMEM((EL, R, FF), BF), pltpu.VMEM((EL, R, FF), BF), pltpu.VMEM((EL, R, FF), BF),
            pltpu.VMEM((NB, EL * RB, 1), F32), pltpu.VMEM((NB, EL * RB, 1), F32),
            pltpu.VMEM((4, ND, TOK, DH), F32), pltpu.VMEM((4, 8, TOK, DH), F32), pltpu.VMEM((4, 2, 7, HALF, DH), F32),
            pltpu.VMEM((ND, EL, 128), F32), pltpu.VMEM((ND, EL, 128), F32),
            dma(2, 2, LAST), dma(2, 2, LAST), dma(2, 2, LAST + 1), dma(2, 2, LAST + 1), dma(ND), dma(ND), dma(ND), dma(ND),
            dma(4, 2, 7), dma(4, 2, 7), dma(4, 8), dma(4, 8),
        ],
        compiler_params=pltpu.CompilerParams(vmem_limit_bytes=VMEM_LIMIT, collective_id=0, has_side_effects=True),
        name='moe',
    )(ridx, gates, x, dy, w1, w3, w2)


def dw_kernel(y, dx, dg, x, do, a, du, dv, yo, dxo, dgo, g1, g3, g2, b1, b3, b2, sem):
    e = pl.program_id(0)
    slot = lax.rem(e, 2)
    xb = x[...].reshape(NB * RB, D)
    made = ((g1, b1, lambda: dot_tn(xb, du[0])), (g3, b3, lambda: dot_tn(xb, dv[0])),
            (g2, b2, lambda: dot_tn(a[0], do[...].reshape(NB * RB, D))))
    for i, (out, buf, make) in enumerate(made):
        @pl.when(e >= 2)
        def _():
            pltpu.make_async_copy(buf.at[slot], out.at[e - 2], sem.at[i, slot]).wait()
        buf[slot] = make()
        pltpu.make_async_copy(buf.at[slot], out.at[e], sem.at[i, slot]).start()

    @pl.when(e == 0)
    def _():
        yo[...] = y[...]
        dxo[...] = dx[...]
        dgo[...] = dg[...]

    @pl.when(e == EL - 1)
    def _():
        for i, (out, buf, make) in enumerate(made):
            pltpu.make_async_copy(buf.at[1 - slot], out.at[e - 1], sem.at[i, 1 - slot]).wait()
            pltpu.make_async_copy(buf.at[slot], out.at[e], sem.at[i, slot]).wait()


def dw(y, dx, dg, xr, dor, ar, dur, dvr):
    sds = jax.ShapeDtypeStruct
    R = NB * RB
    whole = lambda *s: pl.BlockSpec(s, lambda e: (0, 0))
    act = pl.BlockSpec((1, R, FF), lambda e: (e, 0, 0))
    br = pl.BlockSpec((NB, RB, D), lambda e: (0, e, 0))
    same = [whole(TOK, D), whole(TOK, D), whole(TOP, TOK)]
    return pl.pallas_call(
        dw_kernel,
        grid=(EL,),
        out_shape=(sds((TOK, D), BF), sds((TOK, D), BF), sds((TOP, TOK), F32),
                   sds((EL, D, FF), F32), sds((EL, D, FF), F32), sds((EL, FF, D), F32)),
        in_specs=same + [br, br, act, act, act],
        out_specs=same + [pl.BlockSpec(memory_space=pl.ANY)] * 3,
        scratch_shapes=[pltpu.VMEM((2, D, FF), F32), pltpu.VMEM((2, D, FF), F32), pltpu.VMEM((2, FF, D), F32),
                        pltpu.SemaphoreType.DMA((3, 2))],
        name='dw',
    )(y, dx, dg, xr, dor, ar, dur, dvr)


def solution(mesh):
    grp = ('row', 'col')
    tspec = P(('dp', 'row', 'col'), None)
    wspec = P(grp, None, None)
    gspec = P(('dp', 'row', 'col'), None, None)

    def local(x, ridx, gates, w1, w3, w2, dy):
        y, dx, dg, g1, g3, g2 = dw(*main(ridx.T, gates.T, x, dy, w1, w3, w2))
        return y, dx, dg.T, g1, g3, g2

    return jax.shard_map(local, mesh=mesh, in_specs=(tspec, tspec, tspec, wspec, wspec, wspec, tspec),
                         out_specs=(tspec, tspec, tspec, gspec, gspec, gspec), check_vma=False)
```

```python
import functools

import jax
import jax.numpy as jnp
from jax import lax
from jax.experimental import pallas as pl
from jax.experimental.pallas import tpu as pltpu
from jax.sharding import PartitionSpec as P

TOK = 64
ND = 16
D = 1024
FF = 384
EL = 8
TOP = 8
CAP = 16
NB = 4
TB = 4 * TOK
RB = 4 * CAP
NT = ND * TOK
BF = jnp.bfloat16
F32 = jnp.float32
VMEM_LIMIT = 67043328


def dot(a, b):
    return lax.dot_general(a, b, (((1,), (0,)), ((), ())), preferred_element_type=F32)


def dot_nt(a, b):
    return lax.dot_general(a, b, (((1,), (1,)), ((), ())), preferred_element_type=F32)


def dot_tn(a, b):
    return lax.dot_general(a, b, (((0,), (0,)), ((), ())), preferred_element_type=F32)


def put_codes(b, base, meta, code, gate):
    m = [meta[NB * b + i] for i in range(NB)]
    route = jnp.concatenate([a[:, :TOK] for a in m], axis=1)
    gates = jnp.concatenate([a[:, TOK:] for a in m], axis=1)
    rows, gr = [], []
    for e in range(EL):
        eq = route == (base + e).astype(F32)
        rows.append(jnp.sum(jnp.where(eq, 1.0, 0.0), axis=0, keepdims=True))
        gr.append(jnp.sum(jnp.where(eq, gates, 0.0), axis=0, keepdims=True))
    mem = jnp.concatenate(rows, axis=0)
    gate[b] = jnp.concatenate(gr, axis=0)
    i0 = lax.broadcasted_iota(jnp.int32, (TB, TB), 0)
    i1 = lax.broadcasted_iota(jnp.int32, (TB, TB), 1)
    upper = jnp.where((i0 < i1) & (i0 // TOK == i1 // TOK), 1.0, 0.0).astype(BF)
    src = lax.broadcasted_iota(jnp.int32, (EL, TB), 1) // TOK * CAP
    rank = dot(mem.astype(BF), upper).astype(jnp.int32)
    code[b] = jnp.where(mem > 0.5, rank + src, -1)


def select(code, b):
    row = lax.broadcasted_iota(jnp.int32, (RB, TB), 0)
    c = code[b]
    return jnp.concatenate([jnp.broadcast_to(c[e:e + 1], (RB, TB)) == row for e in range(EL)], axis=0)


def spread(gate, b):
    g = gate[b]
    return jnp.concatenate([jnp.broadcast_to(g[e:e + 1], (RB, TB)) for e in range(EL)], axis=0)


def put_tables(b, code, gate, gs, tab):
    lane = lax.broadcasted_iota(jnp.int32, (EL, EL * RB), 1)
    widen = jnp.where(lane // RB == lax.broadcasted_iota(jnp.int32, (EL, EL * RB), 0), 1.0, 0.0).astype(BF)
    row = (lax.broadcasted_iota(jnp.int32, (TB, EL * RB), 1) % RB).astype(F32)
    sel = dot_tn(code[b].astype(F32).astype(BF), widen) == row
    g = gate[b]
    for i in range(3):
        part = g.astype(BF)
        g = g - part.astype(F32)
        tab[b, i] = jnp.where(sel, dot_tn(part, widen), 0.0).astype(BF)
    tab[b, 3] = jnp.where(sel, 1.0, 0.0).astype(BF)
    gs[b] = jnp.sum(jnp.where(select(code, b), spread(gate, b), 0.0), axis=1, keepdims=True)


def place(pos, core):
    y = pos // 4
    return pos + y * (7 - 2 * pos), 2 * y + core


def remote(src, dst, ss, rs, dev):
    return pltpu.make_async_remote_copy(
        src_ref=src, dst_ref=dst, send_sem=ss, recv_sem=rs,
        device_id={'row': dev[0], 'col': dev[1]}, device_id_type=pl.DeviceIdType.MESH)


QR = TOK // 4
NR = 14
NC = 4
CH = TOK // NC
LAST = 3 * NC + NC // 2
DH = D // 2
PEERS = [(o, k) for o in range(8) for k in range(2)][1:]


def main_kernel(ridxh, gatesh, x, dy, w1h, w3h, w2h, yo, dxo, dgo, xrh, dorh, arh, durh, dvrh,
                w1, w3, w2, wsem, osem, isem, ridx, gates, meta, xg, dyg, mg, code, gate, tab, xrow, orow, us, vs, av, gs, ds,
                acc, pbuf, rbuf, dgs, dgr,
                ags, agr, pgs, pgr, ms, mr, gss, gsr, rss, rsr, rps, rpr):
    z = lax.axis_index('row')
    c4 = lax.axis_index('col')
    yy = c4 // 2
    core = c4 % 2
    r = z + yy * (7 - 2 * z)
    base = (z * 4 + c4) * EL
    nbr = (place((r + 1) % 8, core), place((r + 7) % 8, core))
    partner = (z, 2 * yy + 1 - core)
    devs = [place((r + o) % 8, core if k == 0 else 1 - core) for o in range(8) for k in range(2)]

    in_x = pltpu.make_async_copy(x, xg.at[0], isem.at[0])
    in_dy = pltpu.make_async_copy(dy, dyg.at[0], isem.at[1])
    in_r = pltpu.make_async_copy(ridxh, ridx, isem.at[2])
    in_g = pltpu.make_async_copy(gatesh, gates, isem.at[3])
    in_r.start()
    in_g.start()
    in_x.start()
    in_dy.start()
    barrier = pltpu.get_barrier_semaphore()
    for o, k in PEERS:
        dev = devs[2 * o + k]
        pl.semaphore_signal(barrier, inc=1, device_id={'row': dev[0], 'col': dev[1]},
                            device_id_type=pl.DeviceIdType.MESH)
    in_r.wait()
    in_g.wait()
    both = jnp.concatenate([ridx[...].astype(F32), gates[...]], axis=1)
    meta[...] = both
    mg[0] = both
    in_x.wait()
    in_dy.wait()
    pl.semaphore_wait(barrier, ND - 1)

    gath = (xg, dyg)

    def own(t, d, m):
        h = m if d == 0 else NC - 1 - m
        rows = slice(h * CH, h * CH + CH)
        return remote(gath[t].at[0, rows], gath[t].at[14 if d == 0 else 2, rows], ags.at[t, d, m], agr.at[t, d, m], nbr[d])

    def piece(d, m):
        k = 1 + lax.div(m, NC)
        h = lax.rem(m, NC) if d == 0 else NC - 1 - lax.rem(m, NC)
        return (8 - k) if d == 0 else k, pl.ds(pl.multiple_of(h * CH, CH), CH)

    def here(t, d, m):
        c = gath[t].at[0, :CH]
        return remote(c, c, ags.at[t, d, m], agr.at[t, d, m], nbr[d])

    def onward(t, d, m):
        o, rows = piece(d, m)
        return remote(gath[t].at[2 * o, rows], gath[t].at[2 * (o - 1 if d == 0 else o + 1), rows],
                      ags.at[t, d, m + NC], agr.at[t, d, m + NC], nbr[d])

    def across(t, d, m):
        o, rows = piece(d, m)
        return remote(gath[t].at[2 * o, rows], gath[t].at[2 * o + 1, rows], pgs.at[t, d, m], pgr.at[t, d, m], partner)

    def crossed(t, d, m):
        c = gath[t].at[0, :CH]
        return remote(c, c, pgs.at[t, d, m], pgr.at[t, d, m], partner)

    def own_across(t):
        return remote(gath[t].at[0], gath[t].at[1], pgs.at[t, 0, LAST], pgr.at[t, 0, LAST], partner)

    def ag_start(t):
        for m in range(NC):
            for d in range(2):
                own(t, d, m).start()
        own_across(t).start()

    def ag_step(t, m):
        for d in range(2):
            here(t, d, m).wait_recv()
            if isinstance(m, int):
                if m < LAST - NC:
                    onward(t, d, m).start()
            else:
                @pl.when(m < LAST - NC)
                def _():
                    onward(t, d, m).start()
            across(t, d, m).start()

    def ag_crossed(t, lo, hi):
        for m in range(lo, hi):
            for d in range(2):
                crossed(t, d, m).wait_recv()

    def meta_copy(o, k):
        return remote(meta, mg.at[2 * ((8 - o) % 8) + k], ms.at[2 * o + k], mr.at[2 * ((8 - o) % 8) + k], devs[2 * o + k])

    def meta_wait(o, k):
        return remote(meta, mg.at[0], ms.at[2 * o + k], mr.at[2 * o + k], devs[2 * o + k])

    for o, k in PEERS:
        meta_copy(o, k).start()
    ag_start(0)

    def gather_block(src, b):
        p = jnp.where(select(code, b), 1.0, 0.0).astype(BF)
        xrow[b] = dot(p, src[pl.ds(NB * b, NB)].reshape(TB, D)).astype(BF)

    def xload(m, _):
        ag_step(0, m)

        @pl.when(m > 0)
        def _():
            load13(m - 1)
        return 0

    def load13(e):
        pltpu.make_async_copy(w1h.at[e], w1.at[e], wsem.at[e, 0]).start()
        pltpu.make_async_copy(w3h.at[e], w3.at[e], wsem.at[e, 1]).start()

    lax.fori_loop(0, 5, xload, 0)
    for o, k in PEERS:
        meta_wait(o, k).wait_recv()

    def xstep(m, _):
        ag_step(0, m)
        load13(m - 1)

        put_codes(m - 5, base, mg, code, gate)
        return 0

    lax.fori_loop(5, 9, xstep, 0)
    ag_step(0, 9)
    ag_start(1)
    put_tables(0, code, gate, gs, tab)
    ag_step(0, 10)
    for e in range(EL):
        pltpu.make_async_copy(w2h.at[e], w2.at[e], wsem.at[e, 2]).start()
    put_tables(1, code, gate, gs, tab)
    ag_step(0, 11)
    put_tables(2, code, gate, gs, tab)
    put_tables(3, code, gate, gs, tab)
    own_across(0).wait_recv()
    ag_crossed(0, 0, NC)
    gather_block(xg, 0)
    ag_step(0, 12)
    ag_crossed(0, NC, 2 * NC)
    gather_block(xg, 3)
    ag_step(0, 13)
    ag_crossed(0, 2 * NC, 3 * NC)
    gather_block(xg, 1)
    ag_step(1, 0)
    ag_step(1, 1)
    ag_crossed(0, 3 * NC, LAST)
    gather_block(xg, 2)
    ag_step(1, 2)
    ag_step(1, 3)

    def rows_of(ref, e):
        return ref[:, pl.ds(pl.multiple_of(e * RB, RB), RB), :]

    def put_rows(ref, e, v):
        ref[:, pl.ds(pl.multiple_of(e * RB, RB), RB), :] = v.reshape(NB, RB, v.shape[-1])

    out_x = pltpu.make_async_copy(xrow, xrh, osem.at[0])
    out_x.start()

    def fwd(e, _):
        pltpu.make_async_copy(w1h.at[e], w1.at[e], wsem.at[e, 0]).wait()
        pltpu.make_async_copy(w3h.at[e], w3.at[e], wsem.at[e, 1]).wait()
        xe = rows_of(xrow, e).reshape(NB * RB, D)
        u = dot(xe, w1[e]).astype(BF)
        v = dot(xe, w3[e]).astype(BF)
        us[e] = u
        vs[e] = v
        uf = u.astype(F32)
        av[e] = (uf * jax.nn.sigmoid(uf) * v.astype(F32)).astype(BF)
        ag_step(1, e + NC)
        return 0

    lax.fori_loop(0, EL, fwd, 0)
    out_a = pltpu.make_async_copy(av, arh, osem.at[1])
    out_a.start()

    def rs_pair(t, o):
        return remote(acc.at[t, 2 * o + 1], pbuf.at[t, o], rps.at[t, o], rpr.at[t, o], partner)

    def rs_join(t, o):
        rs_pair(t, o).wait_recv()
        acc[t, 2 * o] = acc[t, 2 * o] + pbuf[t, o]

    def rs_got(t, d, q):
        return remote(acc.at[0, 0, :QR], rbuf.at[0, 0, 0], rss.at[t, d, q], rsr.at[t, d, q], nbr[d])

    def rs_move(t, d, q):
        dist = 4 - (q + 2) // 4
        h = q % 4 if d == 0 else 3 - q % 4
        o = dist if d == 0 else 8 - dist
        rows = slice(h * QR, h * QR + QR)
        return 2 * o, rows, remote(acc.at[t, 2 * o, rows], rbuf.at[t, d, q], rss.at[t, d, q], rsr.at[t, d, q], nbr[d])

    def rs_first(t):
        rs_join(t, 4)
        for q in range(2):
            for d in range(2):
                rs_move(t, d, q)[2].start()
        rs_join(t, 3)
        rs_join(t, 5)
        for q in range(2, 4):
            for d in range(2):
                rs_move(t, d, q)[2].start()

    def rs_rest(t):
        for o in (2, 6, 1, 7, 0):
            rs_join(t, o)

    def rs_step(t, m):
        for q in (2 * m, 2 * m + 1):
            for d in range(2):
                rs_got(t, d, q - 4).wait_recv()
                p, rows, copy = rs_move(t, d, q)
                acc[t, p, rows] = acc[t, p, rows] + rbuf[t, d, q - 4]
                copy.start()

    def rs_last(t, out):
        cols = slice((t % 2) * DH, (t % 2) * DH + DH)
        for q in range(NR - 4, NR):
            for d in range(2):
                rs_got(t, d, q).wait_recv()
        for j, (qr, ql) in enumerate(((12, 11), (13, 10), (10, 13), (11, 12))):
            rows = slice(j * QR, j * QR + QR)
            out[rows, cols] = (acc[t, 0, rows] + rbuf[t, 0, qr] + rbuf[t, 1, ql]).astype(BF)

    def forward_half(c):
        cols = slice(c * DH, c * DH + DH)

        def out(e, _):
            if c == 0:
                pltpu.make_async_copy(w2h.at[e], w2.at[e], wsem.at[e, 2]).wait()
            orow[:, pl.ds(pl.multiple_of(e * RB, RB), RB), cols] = dot(av[e], w2[e, :, cols]).astype(BF).reshape(NB, RB, DH)
            if c == 1:
                @pl.when(e == 4)
                def _():
                    rs_rest(0)
            return 0

        lax.fori_loop(0, EL, out, 0)
        if c == 0:
            ag_step(1, 12)
            ag_step(1, 13)

        def scatter(i, _):
            b = lax.rem(3 * i + 2, NB)
            o = orow[b, :, cols]
            acc[c, pl.ds(NB * b, NB)] = (dot(tab[b, 0], o) + dot(tab[b, 1], o) + dot(tab[b, 2], o)).reshape(NB, TOK, DH)
            rs_pair(c, 2 * b).start()
            rs_pair(c, 2 * b + 1).start()
            if c == 1:
                for at, m in ((1, 2), (3, 3)):
                    @pl.when(i == at)
                    def _():
                        rs_step(0, m)
            return 0

        lax.fori_loop(0, NB, scatter, 0)
        rs_first(c)

    forward_half(0)
    forward_half(1)
    own_across(1).wait_recv()
    ag_crossed(1, 0, LAST)
    out_x.wait()

    def gather_dy(b, _):
        gather_block(dyg, b)

        @pl.when(b == 2)
        def _():
            rs_rest(1)
        return 0

    lax.fori_loop(0, NB, gather_dy, 0)
    rs_step(0, 4)

    def bwd(e, _):
        dye = rows_of(xrow, e).reshape(NB * RB, D).astype(F32)
        o = rows_of(orow, e).reshape(NB * RB, D).astype(F32)
        put_rows(ds, e, jnp.sum(dye * o, axis=1, keepdims=True))
        g = rows_of(gs, e).reshape(NB * RB, 1)
        do = (g * dye).astype(BF)
        put_rows(xrow, e, do)
        da = dot_nt(do, w2[e])
        u = us[e].astype(F32)
        v = vs[e].astype(F32)
        s = jax.nn.sigmoid(u)
        du = (da * v * s * (1.0 + u * (1.0 - s))).astype(BF)
        dv = (da * u * s).astype(BF)
        us[e] = du
        vs[e] = dv
        for at, t, m in ((1, 0, 5), (3, 1, 2), (5, 1, 3), (7, 0, 6)):
            @pl.when(e == at)
            def _():
                rs_step(t, m)
        return 0

    lax.fori_loop(0, EL, bwd, 0)
    outs = [pltpu.make_async_copy(xrow, dorh, osem.at[2]), pltpu.make_async_copy(us, durh, osem.at[3]),
            pltpu.make_async_copy(vs, dvrh, osem.at[4])]
    for c in outs:
        c.start()

    def backward_half(c):
        cols = slice(c * DH, c * DH + DH)

        def back(e, _):
            dx = dot_nt(us[e], w1[e, cols, :]) + dot_nt(vs[e], w3[e, cols, :])
            orow[:, pl.ds(pl.multiple_of(e * RB, RB), RB), cols] = dx.astype(BF).reshape(NB, RB, DH)
            if c == 0:
                for at, m in ((3, 4), (7, 5)):
                    @pl.when(e == at)
                    def _():
                        rs_step(1, m)
            else:
                @pl.when(e == 3)
                def _():
                    rs_rest(2)

                @pl.when(e == 7)
                def _():
                    rs_step(2, 2)
            return 0

        lax.fori_loop(0, EL, back, 0)

        def scatter(i, _):
            b = lax.rem(3 * i + 2, NB)
            acc[2 + c, pl.ds(NB * b, NB)] = dot(tab[b, 3], orow[b, :, cols]).reshape(NB, TOK, DH)
            rs_pair(2 + c, 2 * b).start()
            rs_pair(2 + c, 2 * b + 1).start()
            if c == 1:
                @pl.when(i == 2)
                def _():
                    rs_step(2, 3)
            return 0

        lax.fori_loop(0, NB, scatter, 0)
        rs_first(2 + c)

    backward_half(0)
    rs_step(1, 6)
    backward_half(1)

    def slots_back(b, _):
        dg = jnp.where(select(code, b), ds[b], 0.0)
        dge = jnp.concatenate([jnp.sum(dg[e * RB:(e + 1) * RB], axis=0, keepdims=True) for e in range(EL)], axis=0)
        for i in range(NB):
            dgs[NB * b + i, :, :TOK] = dge[:, i * TOK:(i + 1) * TOK]
        return 0

    lax.fori_loop(0, NB, slots_back, 0)

    def dg_copy(o, k):
        return remote(dgs.at[2 * o + k], dgr.at[2 * ((8 - o) % 8) + k], gss.at[2 * o + k], gsr.at[2 * ((8 - o) % 8) + k],
                      devs[2 * o + k])

    def dg_wait(o, k):
        return remote(dgs.at[0], dgr.at[0], gss.at[2 * o + k], gsr.at[2 * o + k], devs[2 * o + k])

    for o, k in PEERS:
        dg_copy(o, k).start()
    dgr[0] = dgs[0]
    rs_rest(3)

    rs_last(0, yo)
    rs_step(2, 4)
    rs_last(1, yo)
    rs_step(2, 5)
    rs_step(3, 2)
    rs_step(3, 3)
    rs_step(2, 6)
    rs_step(3, 4)
    rs_step(3, 5)
    for t in range(2):
        own_across(t).wait_send()
        for m in range(LAST):
            for d in range(2):
                here(t, d, m).wait_send()
                crossed(t, d, m).wait_send()
    for o, k in PEERS:
        meta_wait(o, k).wait_send()
    out_a.wait()
    for c in outs:
        c.wait()
    for t in range(4):
        for o in range(8):
            rs_pair(t, o).wait_send()
    rs_step(3, 6)
    for t in range(2):
        for q in range(NR):
            for d in range(2):
                rs_got(t, d, q).wait_send()
    rs_last(2, dxo)
    rs_last(3, dxo)
    for o, k in PEERS:
        dg_wait(o, k).wait_recv()
    lane = lax.broadcasted_iota(jnp.int32, (EL, TOK), 0)
    total = [jnp.zeros((EL, TOK), F32)] * TOP
    for i in range(ND):
        expert = lane + (devs[i][0] * 4 + devs[i][1]) * EL
        back = dgr[i, :, :TOK]
        total = [t + jnp.where(expert == ridx[j:j + 1], back, 0.0) for j, t in enumerate(total)]
    dgo[...] = jnp.concatenate([jnp.sum(t, axis=0, keepdims=True) for t in total], axis=0)
    for o, k in PEERS:
        dg_wait(o, k).wait_send()
    for t in range(2, 4):
        for q in range(NR):
            for d in range(2):
                rs_got(t, d, q).wait_send()


def main(ridx, gates, x, dy, w1, w3, w2):
    vm = pl.BlockSpec(memory_space=pltpu.VMEM)
    hb = pl.BlockSpec(memory_space=pl.ANY)
    sds = jax.ShapeDtypeStruct
    R = NB * RB
    dma = lambda *s: pltpu.SemaphoreType.DMA(s)
    return pl.pallas_call(
        main_kernel,
        out_shape=(sds((TOK, D), BF), sds((TOK, D), BF), sds((TOP, TOK), F32),
                   sds((NB, EL * RB, D), BF), sds((NB, EL * RB, D), BF), sds((EL, R, FF), BF), sds((EL, R, FF), BF), sds((EL, R, FF), BF)),
        in_specs=[hb] * 7,
        out_specs=[vm, vm, vm] + [hb] * 5,
        scratch_shapes=[
            pltpu.VMEM((EL, D, FF), BF), pltpu.VMEM((EL, D, FF), BF), pltpu.VMEM((EL, FF, D), BF),
            dma(EL, 3), dma(5), dma(4), pltpu.VMEM((TOP, TOK), jnp.int32), pltpu.VMEM((TOP, TOK), F32), pltpu.VMEM((TOP, 128), F32),
            pltpu.VMEM((ND, TOK, D), BF), pltpu.VMEM((ND, TOK, D), BF), pltpu.VMEM((ND, TOP, 128), F32),
            pltpu.VMEM((NB, EL, TB), jnp.int32), pltpu.VMEM((NB, EL, TB), F32), pltpu.VMEM((NB, 4, TB, EL * RB), BF),
            pltpu.VMEM((NB, EL * RB, D), BF), pltpu.VMEM((NB, EL * RB, D), BF),
            pltpu.VMEM((EL, R, FF), BF), pltpu.VMEM((EL, R, FF), BF), pltpu.VMEM((EL, R, FF), BF),
            pltpu.VMEM((NB, EL * RB, 1), F32), pltpu.VMEM((NB, EL * RB, 1), F32),
            pltpu.VMEM((4, ND, TOK, DH), F32), pltpu.VMEM((4, 8, TOK, DH), F32), pltpu.VMEM((4, 2, NR, QR, DH), F32),
            pltpu.VMEM((ND, EL, 128), F32), pltpu.VMEM((ND, EL, 128), F32),
            dma(2, 2, LAST), dma(2, 2, LAST), dma(2, 2, LAST + 1), dma(2, 2, LAST + 1), dma(ND), dma(ND), dma(ND), dma(ND),
            dma(4, 2, NR), dma(4, 2, NR), dma(4, 8), dma(4, 8),
        ],
        compiler_params=pltpu.CompilerParams(vmem_limit_bytes=VMEM_LIMIT, collective_id=0, has_side_effects=True),
        name='moe',
    )(ridx, gates, x, dy, w1, w3, w2)


def dw_kernel(y, dx, dg, x, do, a, du, dv, yo, dxo, dgo, g1, g3, g2):
    @pl.when(pl.program_id(0) == 0)
    def _():
        yo[...] = y[...]
        dxo[...] = dx[...]
        dgo[...] = dg[...]
    xb = x[...].reshape(NB * RB, D)
    g1[0] = dot_tn(xb, du[0])
    g3[0] = dot_tn(xb, dv[0])
    g2[0] = dot_tn(a[0], do[...].reshape(NB * RB, D))


def dw(y, dx, dg, xr, dor, ar, dur, dvr):
    sds = jax.ShapeDtypeStruct
    R = NB * RB
    whole = lambda *s: pl.BlockSpec(s, lambda e: (0, 0))
    act = pl.BlockSpec((1, R, FF), lambda e: (e, 0, 0))
    br = pl.BlockSpec((NB, RB, D), lambda e: (0, e, 0))
    same = [whole(TOK, D), whole(TOK, D), whole(TOP, TOK)]
    return pl.pallas_call(
        dw_kernel,
        grid=(EL,),
        out_shape=(sds((TOK, D), BF), sds((TOK, D), BF), sds((TOP, TOK), F32),
                   sds((EL, D, FF), F32), sds((EL, D, FF), F32), sds((EL, FF, D), F32)),
        in_specs=same + [br, br, act, act, act],
        out_specs=same + [pl.BlockSpec((1, D, FF), lambda e: (e, 0, 0)), pl.BlockSpec((1, D, FF), lambda e: (e, 0, 0)),
                          pl.BlockSpec((1, FF, D), lambda e: (e, 0, 0))],
        name='dw',
    )(y, dx, dg, xr, dor, ar, dur, dvr)


def solution(mesh):
    grp = ('row', 'col')
    tspec = P(('dp', 'row', 'col'), None)
    wspec = P(grp, None, None)
    gspec = P(('dp', 'row', 'col'), None, None)

    def local(x, ridx, gates, w1, w3, w2, dy):
        y, dx, dg, g1, g3, g2 = dw(*main(ridx.T, gates.T, x, dy, w1, w3, w2))
        return y, dx, dg.T, g1, g3, g2

    return jax.shard_map(local, mesh=mesh, in_specs=(tspec, tspec, tspec, wspec, wspec, wspec, tspec),
                         out_specs=(tspec, tspec, tspec, gspec, gspec, gspec), check_vma=False)
```
